32 devices in a mesh: dp: 8 (over y, x, core), shard: 4 (over z).
Axes of the slice: x: 2, y: 2, z: 4, core: 2. Of those that a mesh axis runs over, the one named last changes fastest.
Arguments:
- block_input: bfloat16 [16384, 768], P(('dp', 'shard')), may hold values from -64 to 64
- cotangent: bfloat16 [16384, 768], P(('dp', 'shard')), may hold values from -4 to 4
- token_bounds: int32 [32, 2], P(('dp', 'shard')), may hold values from 0 to 11426, as said below
- params: float32 [7087104], P('shard'), may hold values from -3 to 3
- first_moment: float32 [7087104], P('shard')
- second_moment: float32 [7087104], P('shard'), as said below
Outputs:
- activations: float32 [16384, 768], P(('dp', 'shard'))
- input_grad: float32 [16384, 768], P(('dp', 'shard'))
- param_grad: float32 [4, 8, 221472], P('shard', 'dp')
- new_params: float32 [7087104], P('shard')
- new_first: float32 [7087104], P('shard')
- new_second: float32 [7087104], P('shard')
The draws below stay inside these ranges and needn't reach their ends.
Inputs may be any that keep to these rules, and one draw needn't show every extreme that they name: `token_bounds`: row d, devices taken in the order of dp then shard, holds the first token and one past the last token of device d among the 11426 tokens in image order. The ranges meet end to start, the first begins at 0 and the last ends at 11426. Every device holds at least 197 and at most 512 tokens, and some device exactly 512. `second_moment`: every entry is positive.
All inputs are finite; a program needn't handle non-finite values.
Results may differ from the reference program's by a relative error of at most 0.02.
The reference program's roundings to bfloat16 on the way count: a program that leaves them out, or rounds other values in their place, can miss the bound.
Values may be sent and summed in bfloat16 or wider, within the bound.
A program may use at most 256 MiB of HBM per device.

```python
import math
import jax
import jax.numpy as jnp
from jax import lax

D = 768
HEADS = 12
HD = 64
FF = 3072
IMG = 197
TOK_DEV = 512
SLOTS = 16384
IMAGES = 58
TOTAL = 11426
PARAMS = 7087104
PIECE = 221472
N_DP = 8
N_SHARD = 4


def layout_noise(key):
    return jax.random.truncated_normal(jax.random.fold_in(key, 11), -4.0, 4.0, (PARAMS,), jnp.float32)


def segment_scale(flat_ids, factors):
    edge_one = 3 * D * D
    edge_two = edge_one + D * D
    edge_three = edge_two + D * FF
    edge_four = edge_three + FF * D
    edge_five = edge_four + 8 * D
    return jnp.where(flat_ids < edge_one, factors[0], jnp.where(flat_ids < edge_two, factors[1], jnp.where(flat_ids < edge_three, factors[2], jnp.where(flat_ids < edge_four, factors[3], jnp.where(flat_ids < edge_five, factors[4], factors[5])))))


def draw_params(key, part):
    base = layout_noise(key)
    flat_ids = jnp.arange(PARAMS, dtype=jnp.int32)
    scales = segment_scale(flat_ids, [D ** (-0.5), (D // 32) ** (-0.5), D ** (-0.5), FF ** (-0.5), 0.3, 0.3])
    values = base * scales
    edge_four = 3 * D * D + D * D + D * FF + FF * D
    edge_five = edge_four + 8 * D
    vec_row = (flat_ids - edge_four) // D
    is_gain = (flat_ids >= edge_four) & (flat_ids < edge_five) & ((vec_row == 0) | (vec_row == 5))
    gains = jax.random.uniform(jax.random.fold_in(key, 13), (PARAMS,), jnp.float32, 0.7, 1.3)
    values = jnp.where(is_gain, gains, values)
    return values


def draw_block_input(key, part):
    row_scale = jnp.exp(jax.random.uniform(jax.random.fold_in(key, 22), (SLOTS, 1), jnp.float32, math.log(0.4), math.log(4.0)))
    col_scale = jnp.exp(jax.random.uniform(jax.random.fold_in(key, 23), (1, D), jnp.float32, math.log(0.4), math.log(4.0)))
    noise = jax.random.truncated_normal(jax.random.fold_in(key, 21), -4.0, 4.0, (SLOTS, D), jnp.float32)
    values = noise * row_scale * col_scale
    return values.astype(jnp.bfloat16)


def state_draws(key):
    flat_ids = jnp.arange(PARAMS, dtype=jnp.int32)
    scales = segment_scale(flat_ids, [1.0, 0.2, 0.4, 0.65, 1.0, 0.4]) * math.sqrt(TOTAL)
    normal = jax.random.truncated_normal(jax.random.fold_in(key, 31), -4.0, 4.0, (PARAMS,), jnp.float32)
    factor = jnp.exp(jax.random.uniform(jax.random.fold_in(key, 32), (PARAMS,), jnp.float32, math.log(0.5), math.log(2.0)))
    return (normal * scales, factor, scales)


def draw_first_moment(key, part):
    prior, factor, scales = state_draws(key)
    return 0.1 * prior


def draw_second_moment(key, part):
    prior, factor, scales = state_draws(key)
    return 0.001 * (prior * prior * factor + 0.1 * scales * scales)


def draw_token_bounds(key, part):
    devices = SLOTS // TOK_DEV
    pairs = devices // 2
    edges = 2 * jnp.arange(pairs + 1, dtype=jnp.int32) * TOTAL // devices
    spans = edges[1:] - edges[:-1]
    cuts = jax.random.randint(jax.random.fold_in(key, 41), (pairs,), spans - TOK_DEV, TOK_DEV + 1)
    forced = jax.random.randint(jax.random.fold_in(key, 42), (), 0, pairs)
    cuts = jnp.where(jnp.arange(pairs, dtype=jnp.int32) == forced, TOK_DEV, cuts)
    middles = edges[:-1] + cuts
    starts = jnp.stack([edges[:-1], middles], axis=1).reshape(devices)
    finishes = jnp.stack([middles, edges[1:]], axis=1).reshape(devices)
    return jnp.stack([starts, finishes], axis=1).astype(jnp.int32)


def block_levels(rng, shape, cuts, least, high):
    def one(axis_at, shards_of):
        draws = jax.random.uniform(jax.random.fold_in(jax.random.fold_in(rng, 6), axis_at), (shards_of,), jnp.float32, least / len(cuts), high / len(cuts))
        return jnp.repeat(jnp.exp(draws), shape[axis_at] // shards_of).reshape((-1,) + (1,) * (len(shape) - axis_at - 1))

    loudness = one(*cuts[0])
    for cut in cuts[1:]:
        loudness = loudness * one(*cut)
    return loudness


def bell_draw(rng, dims, scale, bound, cuts=(), kind=jnp.bfloat16):
    factor_of = block_levels(rng, dims, cuts, -0.22, 0.18) if cuts else 1.0
    entries = jax.random.normal(rng, dims, jnp.float32) * scale * factor_of
    return jnp.minimum(jnp.maximum(entries, -bound), bound).astype(kind)


def setup_inputs(seed: int = 0) -> dict:
    seeds = jax.random.split(jax.random.key(seed), 7)
    block_input = draw_block_input(jax.random.fold_in(seeds[6], 71), 0)
    cotangent = bell_draw(seeds[1], (SLOTS, D), 1.0, 4.0, ((0, 32),))
    token_bounds = draw_token_bounds(jax.random.fold_in(seeds[6], 71), 0)
    params = draw_params(jax.random.fold_in(seeds[6], 71), 0)
    first_moment = draw_first_moment(jax.random.fold_in(seeds[6], 71), 0)
    second_moment = draw_second_moment(jax.random.fold_in(seeds[6], 71), 0)
    return dict(block_input=block_input, cotangent=cotangent, token_bounds=token_bounds, params=params, first_moment=first_moment, second_moment=second_moment)


ln_eps = 1e-06
beta_one = 0.9
beta_two = 0.999
learn_rate = 0.02
decay_rate = 0.05
adam_eps = 1e-08
image_group = 16
sqrt_half = 0.7071067811865476
inv_root_two_pi = 0.3989422804014327

def widen(array_in):
    return lax.optimization_barrier(array_in).astype(jnp.float32)

def gelu_value(preact):
    return 0.5 * preact * (1.0 + lax.erf(preact * sqrt_half))

def gelu_slope(preact):
    return 0.5 * (1.0 + lax.erf(preact * sqrt_half)) + preact * jnp.exp(-0.5 * preact * preact) * inv_root_two_pi

def norm_forward(values, gain_vec, shift_vec):
    centre = lax.optimization_barrier(jnp.mean(values, axis=-1, keepdims=True))
    centred = values - centre
    spread = lax.optimization_barrier(jnp.mean(centred * centred, axis=-1, keepdims=True))
    inverse = lax.rsqrt(spread + ln_eps)
    normed = centred * inverse
    return (normed * gain_vec + shift_vec, normed, inverse)

def norm_backward(upstream, normed, inverse, gain_vec):
    scaled = upstream * gain_vec
    first_mean = lax.optimization_barrier(jnp.mean(scaled, axis=-1, keepdims=True))
    second = lax.optimization_barrier(jnp.mean(scaled * normed, axis=-1, keepdims=True))
    return inverse * (scaled - first_mean - normed * second)

def unpack(flat_vec):
    lengths = [3 * D * D, D * D, D * FF, FF * D, 8 * D, FF]
    pieces = []
    cursor = 0
    for extent in lengths:
        pieces.append(flat_vec[cursor:cursor + extent])
        cursor = cursor + extent
    return (pieces[0].reshape(D, 3 * D), pieces[1].reshape(D, D), pieces[2].reshape(D, FF), pieces[3].reshape(FF, D), pieces[4].reshape(8, D), pieces[5])

def reference(block_input, cotangent, token_bounds, params, first_moment, second_moment):
    weight_qkv, weight_out, weight_in, weight_back, vectors, bias_raw = unpack(params.astype(jnp.bfloat16))
    vector_f = vectors.astype(jnp.float32)
    bias_in = bias_raw.astype(jnp.float32)
    gain_one, shift_one, bias_q, bias_v = (vector_f[0], vector_f[1], vector_f[2], vector_f[3])
    bias_out, gain_two, shift_two, bias_back = (vector_f[4], vector_f[5], vector_f[6], vector_f[7])
    slot_ids = jnp.arange(SLOTS, dtype=jnp.int32)
    owners = slot_ids // TOK_DEV
    offsets = slot_ids - owners * TOK_DEV
    starts = jnp.take(token_bounds[:, 0], owners)
    finishes = jnp.take(token_bounds[:, 1], owners)
    is_live = offsets < finishes - starts
    groups = (IMAGES + image_group - 1) // image_group
    padded = groups * image_group * IMG
    target = jnp.where(is_live, starts + offsets, padded).astype(jnp.int32)
    stream_all = jnp.zeros((padded, D), jnp.float32).at[target].set(block_input.astype(jnp.float32), mode='drop')
    tangent_all = jnp.zeros((padded, D), jnp.float32).at[target].set(cotangent.astype(jnp.float32), mode='drop')
    group_rows = image_group * IMG
    shape_four = (image_group, IMG, HEADS, HD)

    def group_step(totals, inputs):
        stream, tangent = inputs
        first_out, first_normed, first_inv = norm_forward(stream, gain_one, shift_one)
        first_feed = first_out.astype(jnp.bfloat16)
        projected = jnp.dot(first_feed, weight_qkv, preferred_element_type=jnp.float32)
        queries = ((projected[:, :D] + bias_q) * 0.125).astype(jnp.bfloat16)
        key_rows = projected[:, D:2 * D].astype(jnp.bfloat16)
        value_rows = (projected[:, 2 * D:] + bias_v).astype(jnp.bfloat16)
        query_four = widen(queries).reshape(shape_four)
        key_four = widen(key_rows).reshape(shape_four)
        value_four = widen(value_rows).reshape(shape_four)
        scores = jnp.einsum('gqhd,gkhd->ghqk', query_four, key_four)
        row_top = lax.optimization_barrier(jnp.max(scores, axis=-1, keepdims=True))
        log_total = row_top + jnp.log(lax.optimization_barrier(jnp.sum(jnp.exp(scores - row_top), axis=-1, keepdims=True)))
        probs_f = jnp.exp(scores - log_total)
        probs_b = probs_f.astype(jnp.bfloat16)
        attended = jnp.einsum('ghqk,gkhd->gqhd', widen(probs_b), value_four).reshape(group_rows, D).astype(jnp.bfloat16)
        middle = stream + jnp.dot(attended, weight_out, preferred_element_type=jnp.float32) + bias_out
        second_out, second_normed, second_inv = norm_forward(middle, gain_two, shift_two)
        second_feed = second_out.astype(jnp.bfloat16)
        preact = jnp.dot(second_feed, weight_in, preferred_element_type=jnp.float32) + bias_in
        activated = gelu_value(preact).astype(jnp.bfloat16)
        result = middle + jnp.dot(activated, weight_back, preferred_element_type=jnp.float32) + bias_back
        tangent_b = tangent.astype(jnp.bfloat16)
        grad_back = jnp.dot(activated.T, tangent_b, preferred_element_type=jnp.float32)
        grad_bias_back = lax.optimization_barrier(jnp.sum(tangent, axis=0))
        slope_in = jnp.dot(tangent_b, weight_back.T, preferred_element_type=jnp.float32) * gelu_slope(preact)
        grad_bias_in = lax.optimization_barrier(jnp.sum(slope_in, axis=0))
        slope_feed = slope_in.astype(jnp.bfloat16)
        grad_in = jnp.dot(second_feed.T, slope_feed, preferred_element_type=jnp.float32)
        back_two = jnp.dot(slope_feed, weight_in.T, preferred_element_type=jnp.float32)
        grad_gain_two = lax.optimization_barrier(jnp.sum(back_two * second_normed, axis=0))
        grad_shift_two = lax.optimization_barrier(jnp.sum(back_two, axis=0))
        middle_grad = tangent + norm_backward(back_two, second_normed, second_inv, gain_two)
        middle_feed = middle_grad.astype(jnp.bfloat16)
        grad_out = jnp.dot(attended.T, middle_feed, preferred_element_type=jnp.float32)
        grad_bias_out = lax.optimization_barrier(jnp.sum(middle_grad, axis=0))
        attended_grad = jnp.dot(middle_feed, weight_out.T, preferred_element_type=jnp.float32).astype(jnp.bfloat16)
        grad_four = widen(attended_grad).reshape(shape_four)
        value_grad = jnp.einsum('ghqk,gqhd->gkhd', widen(probs_b), grad_four)
        prob_grad = jnp.einsum('gqhd,gkhd->ghqk', grad_four, value_four)
        centre_term = lax.optimization_barrier(jnp.sum(grad_four * widen(attended).reshape(shape_four), axis=-1))
        centre_term = jnp.transpose(centre_term, (0, 2, 1))[..., None]
        score_grad = (probs_f * (prob_grad - centre_term)).astype(jnp.bfloat16)
        score_wide = widen(score_grad)
        query_grad = jnp.einsum('ghqk,gkhd->gqhd', score_wide, key_four).reshape(group_rows, D) * 0.125
        key_grad = jnp.einsum('ghqk,gqhd->gkhd', score_wide, query_four).reshape(group_rows, D)
        value_grad = value_grad.reshape(group_rows, D)
        grad_bias_q = lax.optimization_barrier(jnp.sum(query_grad, axis=0))
        grad_bias_v = lax.optimization_barrier(jnp.sum(value_grad, axis=0))
        joined = jnp.concatenate([query_grad, key_grad, value_grad], axis=1).astype(jnp.bfloat16)
        grad_qkv = jnp.dot(first_feed.T, joined, preferred_element_type=jnp.float32)
        back_one = jnp.dot(joined, weight_qkv.T, preferred_element_type=jnp.float32)
        grad_gain_one = lax.optimization_barrier(jnp.sum(back_one * first_normed, axis=0))
        grad_shift_one = lax.optimization_barrier(jnp.sum(back_one, axis=0))
        stream_grad = middle_grad + norm_backward(back_one, first_normed, first_inv, gain_one)
        vector_grad = jnp.stack([grad_gain_one, grad_shift_one, grad_bias_q, grad_bias_v, grad_bias_out, grad_gain_two, grad_shift_two, grad_bias_back])
        fresh = (grad_qkv, grad_out, grad_in, grad_back, vector_grad, grad_bias_in)
        totals = tuple((old + new for old, new in zip(totals, fresh)))
        return (totals, (result, stream_grad))
    zero_grads = (jnp.zeros((D, 3 * D), jnp.float32), jnp.zeros((D, D), jnp.float32), jnp.zeros((D, FF), jnp.float32), jnp.zeros((FF, D), jnp.float32), jnp.zeros((8, D), jnp.float32), jnp.zeros((FF,), jnp.float32))
    totals, (outputs, backs) = lax.scan(group_step, zero_grads, (stream_all.reshape(groups, group_rows, D), tangent_all.reshape(groups, group_rows, D)))
    safe_rows = jnp.minimum(target, padded - 1)
    activations = jnp.where(is_live[:, None], jnp.take(outputs.reshape(padded, D), safe_rows, axis=0), 0.0)
    input_grad = jnp.where(is_live[:, None], jnp.take(backs.reshape(padded, D), safe_rows, axis=0), 0.0)
    grad_flat = jnp.concatenate([piece.reshape(-1) for piece in totals])
    matrices = 4 * D * D + 2 * D * FF
    decays = (jnp.arange(PARAMS, dtype=jnp.int32) < matrices).astype(jnp.float32)
    new_first = beta_one * first_moment + (1.0 - beta_one) * grad_flat
    new_second = beta_two * second_moment + (1.0 - beta_two) * grad_flat * grad_flat
    first_hat = new_first / (1.0 - beta_one ** 3)
    second_hat = new_second / (1.0 - beta_two ** 3)
    new_params = params - learn_rate * (first_hat / (jnp.sqrt(second_hat) + adam_eps) + decay_rate * decays * params)
    param_grad = grad_flat.reshape(N_SHARD, N_DP, PIECE)
    return (activations, input_grad, param_grad, new_params, new_first, new_second)
```

```python
import functools

import jax
import jax.numpy as jnp
from jax import lax
from jax.experimental import pallas as pl
from jax.experimental.pallas import tpu as pltpu
from jax.sharding import PartitionSpec as P

D = 768
HEADS = 12
HD = 64
FF = 3072
IMG = 197
BLOCK = 512
HALO = 196
KEY_SPAN = 1024


ln_eps = 1e-06
masked = -1e30
beta_one = 0.9
beta_two = 0.999
learn_rate = 0.02
decay_rate = 0.05
adam_eps = 1e-08
sqrt_half = 0.7071067811865476
inv_root_two_pi = 0.3989422804014327


MESH = pl.DeviceIdType.MESH
LANES = 128
MARGIN = 64


def geometry(n_dp, n_shard):
    total = 4 * D * D + 2 * D * FF + 8 * D + FF
    shard_lines = total // n_shard // LANES
    piece = -(-shard_lines // n_dp // 32) * 32
    piece = -(-(-(-shard_lines // n_dp)) // 32) * 32
    return shard_lines, piece, piece * n_dp


def bit_list(n_dp):
    count = n_dp.bit_length() - 1
    return count, [list(range(1, count)), list(range(count - 1, 0, -1))]


def bits_of(index, count):
    return [lax.rem(lax.div(index, 1 << b), 2) for b in range(count)]


def flipped(index, bits, which):
    return index + sum((1 << b) * (1 - 2 * bits[b]) for b in which)


def greet(n_dp, n_shard, place, level, bits):
    barrier = pltpu.get_barrier_semaphore()
    peers = [(place, lax.rem(level + j, n_shard)) for j in range(1, n_shard)]
    peers += [(flipped(place, bits, [b]), level) for b in range(len(bits))]
    for peer in peers:
        pl.semaphore_signal(barrier, inc=1, device_id=peer, device_id_type=MESH)
    pl.semaphore_wait(barrier, len(peers))


def subsets(order):
    found = [[]]
    for b in order:
        found = found + [kept + [b] for kept in found]
    return found


def gather_kernel(n_dp, n_shard, half, own, out, z_send, z_recv, d_send, d_recv):
    place = lax.axis_index("dp")
    level = lax.axis_index("shard")
    count, orders = bit_list(n_dp)
    bits = bits_of(place, count)
    greet(n_dp, n_shard, place, level, bits)
    started = []

    def push(src, dst, send, recv, target):
        copy = pltpu.make_async_remote_copy(
            src_ref=src,
            dst_ref=dst,
            send_sem=send,
            recv_sem=recv,
            device_id=target,
            device_id_type=MESH,
        )
        copy.start()
        started.append(copy)

    for side in range(2):
        for j in range(1, n_shard):
            push(
                own.at[place, side],
                out.at[level, place, side],
                z_send.at[j - 1, side],
                z_recv.at[j - 1, side],
                (place, lax.rem(level + j, n_shard)),
            )
    chunks = [(j, side) for j in range(1, n_shard) for side in range(2)]

    def advance(chunk, stage):
        j, side = chunks[chunk]
        source = lax.rem(level - j + n_shard, n_shard)
        order = orders[side] + [0]

        def arrived(piece, sem):
            pltpu.make_async_remote_copy(
                src_ref=own.at[place, side],
                dst_ref=out.at[source, piece, side],
                send_sem=z_send.at[0, 0],
                recv_sem=sem,
                device_id=(place, level),
                device_id_type=MESH,
            ).wait_recv()

        if stage == 0:
            arrived(place, z_recv.at[j - 1, side])
        else:
            partner = flipped(place, bits, [order[stage - 1]])
            for slot, which in enumerate(subsets(order[: stage - 1])):
                arrived(
                    flipped(place, bits, which + [order[stage - 1]]),
                    d_recv.at[chunk, (1 << (stage - 1)) - 1 + slot],
                )
        if stage < count:
            partner = flipped(place, bits, [order[stage]])
            for slot, which in enumerate(subsets(order[:stage])):
                piece = flipped(place, bits, which)
                index = (1 << stage) - 1 + slot
                push(
                    out.at[source, piece, side],
                    out.at[source, piece, side],
                    d_send.at[chunk, index],
                    d_recv.at[chunk, index],
                    (partner, level),
                )

    for tick in range(len(chunks) + count):
        for stage in range(count + 1):
            chunk = tick - stage
            if 0 <= chunk < len(chunks):
                advance(chunk, stage)
    for copy in started:
        copy.wait_send()


def gather_weights(n_dp, n_shard, own):
    shard_lines, piece, padded = geometry(n_dp, n_shard)
    half = piece // 2
    chunks = 2 * (n_shard - 1)
    return pl.pallas_call(
        functools.partial(gather_kernel, n_dp, n_shard, half),
        out_shape=jax.ShapeDtypeStruct((n_shard, n_dp, 2, half, LANES), jnp.bfloat16),
        in_specs=[pl.BlockSpec(memory_space=pltpu.HBM)],
        out_specs=pl.BlockSpec(memory_space=pltpu.HBM),
        scratch_shapes=[
            pltpu.SemaphoreType.DMA((n_shard - 1, 2)),
            pltpu.SemaphoreType.DMA((n_shard - 1, 2)),
            pltpu.SemaphoreType.DMA((chunks, n_dp - 1)),
            pltpu.SemaphoreType.DMA((chunks, n_dp - 1)),
        ],
        compiler_params=pltpu.CompilerParams(collective_id=1, has_side_effects=True),
        name="gather_weights",
    )(own)


def weight_plan(n_shard, shard_lines):
    sizes = [(D, 3 * D), (D, D), (D, FF), (FF, D)]
    plan = [[] for _ in range(n_shard)]
    cursor = 0
    for which, (rows, columns) in enumerate(sizes):
        width = columns // LANES
        first = 0
        for s in range(n_shard):
            stop = (s + 1) * shard_lines
            last = min(rows, max(first, (stop - cursor) // width))
            last = last if last == rows else last // 128 * 128
            if last > first:
                plan[s].append((which, first, last, width, cursor + first * width - s * shard_lines))
                first = last
        cursor += rows * width
    return plan, cursor


def layout_kernel(n_shard, shard_lines, padded, own, got, wqkv, wout, win, wback, vec, raw, wide, sem):
    level = lax.axis_index("shard")
    plan, tail = weight_plan(n_shard, shard_lines)
    targets = [wqkv, wout, win, wback]

    def load(s, slot):
        @pl.when(level == s)
        def _():
            pltpu.make_async_copy(own, raw.at[slot], sem.at[slot]).start()

        @pl.when(level != s)
        def _():
            pltpu.make_async_copy(got.at[s], raw.at[slot], sem.at[slot]).start()

    load(0, 0)
    for s in range(n_shard):
        slot = s % 2
        pltpu.make_async_copy(own, raw.at[slot], sem.at[slot]).wait()
        if s + 1 < n_shard:
            load(s + 1, 1 - slot)
        if s:
            wide[0:MARGIN, :] = wide[shard_lines : shard_lines + MARGIN, :]

        def spread(i, carry):
            at = pl.multiple_of(i * 128, 128)
            wide[pl.ds(MARGIN + at, 128), :] = raw[slot, pl.ds(at, 128), :].astype(jnp.float32)
            return carry

        lax.fori_loop(0, padded // 128, spread, 0)
        for which, first, last, width, offset in plan[s]:
            target = targets[which]

            def rows(i, carry):
                at = pl.multiple_of(first + i * 16, 16)
                line = MARGIN + offset + i * (16 * width)
                for c in range(width):
                    target[pl.ds(at, 16), c * LANES : (c + 1) * LANES] = wide[
                        pl.ds(line + c, 16, stride=width), :
                    ].astype(jnp.bfloat16)
                return carry

            lax.fori_loop(0, (last - first) // 16, rows, 0)
    start = MARGIN + tail - (n_shard - 1) * shard_lines
    vec[...] = wide[start : start + vec.shape[0], :]


def lay_out_weights(n_dp, n_shard, own, got):
    shard_lines, piece, padded = geometry(n_dp, n_shard)
    count = (8 * D + FF) // LANES
    shapes = [(D, 3 * D), (D, D), (D, FF), (FF, D)]
    return pl.pallas_call(
        functools.partial(layout_kernel, n_shard, shard_lines, padded),
        out_shape=[jax.ShapeDtypeStruct(shape, jnp.bfloat16) for shape in shapes]
        + [jax.ShapeDtypeStruct((count, LANES), jnp.float32)],
        in_specs=[pl.BlockSpec(memory_space=pltpu.HBM)] * 2,
        out_specs=[pl.BlockSpec(memory_space=pltpu.VMEM)] * 5,
        scratch_shapes=[
            pltpu.VMEM((2, padded, LANES), jnp.bfloat16),
            pltpu.VMEM((MARGIN + padded, LANES), jnp.float32),
            pltpu.SemaphoreType.DMA((2,)),
        ],
        compiler_params=pltpu.CompilerParams(vmem_limit_bytes=60 << 20),
        name="lay_out_weights",
    )(own.reshape(padded, LANES), got.reshape(n_shard, padded, LANES))


def weight_grad_kernel(
    n_shard, shard_lines, padded, feed_one, joined, attended, middle, feed_two, slope, activated, tangent, vec, out, wide, narrow, sem
):
    lefts = [feed_one, attended, feed_two, activated]
    rights = [joined, middle, slope, tangent]
    sizes = [(D, 3 * D), (D, D), (D, FF), (FF, D)]
    cursor = 0
    plan = [[] for _ in range(n_shard)]
    for which, (rows, columns) in enumerate(sizes):
        width = columns // LANES
        for s in range(n_shard):
            begin, stop = s * shard_lines, (s + 1) * shard_lines
            first = max(0, (begin - cursor) // width)
            last = min(rows, -(-(stop - cursor) // width))
            if last > first:
                first = first // 128 * 128
                plan[s].append((which, first, last, width, cursor - begin))
        cursor += rows * width
    tail = cursor - (n_shard - 1) * shard_lines

    def product(which, row, width, group):
        return lax.dot_general(
            lefts[which][:, pl.ds(row, 128)],
            rights[which][:, group * 768 : (group + 1) * 768],
            (((0,), (0,)), ((), ())),
            preferred_element_type=jnp.float32,
        )

    for s in range(n_shard):
        for which, first, last, width, offset in plan[s]:
            full = (last - first) // 128

            def block(i, carry):
                row = pl.multiple_of(first + i * 128, 128)
                line = MARGIN + offset + row * width
                for group in range(width // 6):
                    tile = product(which, row, width, group)
                    for c in range(6):
                        wide[pl.ds(line + group * 6 + c, 128, stride=width), :] = tile[
                            :, c * LANES : (c + 1) * LANES
                        ]
                return carry

            if full:
                lax.fori_loop(0, full, block, 0)
            row = first + full * 128
            rest = -(-(last - row) // 8) * 8
            if rest:
                line = MARGIN + offset + row * width
                for group in range(width // 6):
                    tile = product(which, row, width, group)
                    for c in range(6):
                        wide[pl.ds(line + group * 6 + c, rest, stride=width), :] = tile[
                            :rest, c * LANES : (c + 1) * LANES
                        ]
        if s == n_shard - 1:
            wide[MARGIN + tail : MARGIN + tail + vec.shape[0], :] = vec[...]
        slot = s % 2
        if s >= 2:
            pltpu.make_async_copy(narrow.at[slot], out.at[s - 2], sem.at[slot]).wait()

        def pack(i, carry):
            at = pl.multiple_of(i * 128, 128)
            narrow[slot, pl.ds(at, 128), :] = wide[pl.ds(MARGIN + at, 128), :].astype(jnp.bfloat16)
            return carry

        lax.fori_loop(0, padded // 128, pack, 0)
        pltpu.make_async_copy(narrow.at[slot], out.at[s], sem.at[slot]).start()
    for s in range(n_shard - 2, n_shard):
        pltpu.make_async_copy(narrow.at[s % 2], out.at[s], sem.at[s % 2]).wait()


def weight_grads(n_dp, n_shard, *operands):
    shard_lines, piece, padded = geometry(n_dp, n_shard)
    return pl.pallas_call(
        functools.partial(weight_grad_kernel, n_shard, shard_lines, padded),
        out_shape=jax.ShapeDtypeStruct((n_shard, padded, LANES), jnp.bfloat16),
        in_specs=[pl.BlockSpec(memory_space=pltpu.VMEM)] * 9,
        out_specs=pl.BlockSpec(memory_space=pltpu.HBM),
        scratch_shapes=[
            pltpu.VMEM((MARGIN + padded + 128, LANES), jnp.float32),
            pltpu.VMEM((2, padded, LANES), jnp.bfloat16),
            pltpu.SemaphoreType.DMA((2,)),
        ],
        compiler_params=pltpu.CompilerParams(vmem_limit_bytes=60 << 20),
        name="weight_grads",
    )(*operands)


def reduce_kernel(n_dp, n_shard, half, grads, out, *scratch):
    count, orders = bit_list(n_dp)
    acc, got_core = scratch[0], scratch[1]
    got_bits = scratch[2 : 1 + count]
    got_z, final = scratch[1 + count : 3 + count]
    load_sem, core_send, core_recv, bit_send, bit_recv, z_send, z_recv, g_send, g_recv, keep_sem = scratch[
        3 + count :
    ]
    place = lax.axis_index("dp")
    level = lax.axis_index("shard")
    bits = bits_of(place, count)
    pairs = n_dp // 2
    chunks = [(j, side) for j in list(range(1, n_shard)) + [0] for side in range(2)]
    step = 176 if half % 176 == 0 else 32
    greet(n_dp, n_shard, place, level, bits)
    started = []

    def push(src, dst, send, recv, target):
        copy = pltpu.make_async_remote_copy(
            src_ref=src,
            dst_ref=dst,
            send_sem=send,
            recv_sem=recv,
            device_id=target,
            device_id_type=MESH,
        )
        copy.start()
        started.append(copy)

    def landed(buffer, sem):
        pltpu.make_async_remote_copy(
            src_ref=buffer,
            dst_ref=buffer,
            send_sem=z_send.at[0, 0],
            recv_sem=sem,
            device_id=(place, level),
            device_id_type=MESH,
        ).wait_recv()

    core = bits[0]
    partner = flipped(place, bits, [0])
    for chunk, (j, side) in enumerate(chunks):
        target = lax.rem(level + j, n_shard)
        for m in range(pairs):
            push(
                grads.at[target, 2 * m + 1 - core, side],
                got_core.at[chunk, m],
                core_send.at[chunk, m],
                core_recv.at[chunk, m],
                (partner, level),
            )
            pltpu.make_async_copy(
                grads.at[target, 2 * m + core, side], acc.at[chunk, m], load_sem.at[chunk, m]
            ).start()

    def add(into, other):
        def body(i, carry):
            at = pl.multiple_of(i * step, 16)
            total = into[pl.ds(at, step), :].astype(jnp.float32) + other[pl.ds(at, step), :].astype(
                jnp.float32
            )
            into[pl.ds(at, step), :] = total.astype(jnp.bfloat16)
            return carry

        lax.fori_loop(0, half // step, body, 0)

    def members(order, stage, flip):
        fixed = order[:stage]
        base = sum((bits[b] if b != flip else 1 - bits[b]) * (1 << (b - 1)) for b in fixed)
        return [base + sum(1 << (b - 1) for b in which) for which in subsets(order[stage:])]

    def advance(chunk, stage):
        j, side = chunks[chunk]
        order = orders[side]
        if stage == 0:
            for m in range(pairs):
                pltpu.make_async_copy(
                    grads.at[0, 2 * m + core, side], acc.at[chunk, m], load_sem.at[chunk, m]
                ).wait()
                landed(got_core.at[chunk, m], core_recv.at[chunk, m])
                add(acc.at[chunk, m], got_core.at[chunk, m])
        else:
            for slot, m in enumerate(members(order, stage, None)):
                buffer = got_bits[stage - 1].at[chunk, slot]
                landed(buffer, bit_recv.at[stage - 1, chunk, slot])
                add(acc.at[chunk, m], buffer)
        if stage < count - 1:
            flip = order[stage]
            target = flipped(place, bits, [flip])
            for slot, m in enumerate(members(order, stage + 1, flip)):
                push(
                    acc.at[chunk, m],
                    got_bits[stage].at[chunk, slot],
                    bit_send.at[stage, chunk, slot],
                    bit_recv.at[stage, chunk, slot],
                    (target, level),
                )
        elif j:
            (m,) = members(order, stage, None)
            push(
                acc.at[chunk, m],
                got_z.at[j - 1, side],
                z_send.at[j - 1, side],
                z_recv.at[j - 1, side],
                (place, lax.rem(level + j, n_shard)),
            )

    for tick in range(len(chunks) + count - 1):
        for stage in range(count):
            chunk = tick - stage
            if 0 <= chunk < len(chunks):
                advance(chunk, stage)

    mine = sum(bits[b] * (1 << (b - 1)) for b in range(1, count))
    keeps = []
    for side in range(2):
        chunk = chunks.index((0, side))
        for j in range(1, n_shard):
            landed(got_z.at[j - 1, side], z_recv.at[j - 1, side])

        def body(i, carry):
            at = pl.multiple_of(i * step, 16)
            total = acc[chunk, mine, pl.ds(at, step), :].astype(jnp.float32)
            for j in range(1, n_shard):
                total = total + got_z[j - 1, side, pl.ds(at, step), :].astype(jnp.float32)
            final[side, pl.ds(at, step), :] = total.astype(jnp.bfloat16)
            return carry

        lax.fori_loop(0, half // step, body, 0)
        keep = pltpu.make_async_copy(final.at[side], out.at[place, side], keep_sem.at[side])
        keep.start()
        keeps.append(keep)
        push(
            final.at[side],
            out.at[place, side],
            g_send.at[side, 0],
            g_recv.at[side, 0],
            (flipped(place, bits, [orders[side][0]]), level),
        )
    for stage in range(1, count + 1):
        for side in range(2):
            order = orders[side] + [0]
            for slot, which in enumerate(subsets(order[: stage - 1])):
                landed(
                    out.at[flipped(place, bits, which + [order[stage - 1]]), side],
                    g_recv.at[side, (1 << (stage - 1)) - 1 + slot],
                )
            if stage < count:
                target = flipped(place, bits, [order[stage]])
                for slot, which in enumerate(subsets(order[:stage])):
                    piece = flipped(place, bits, which)
                    index = (1 << stage) - 1 + slot
                    push(
                        final.at[side] if not which else out.at[piece, side],
                        out.at[piece, side],
                        g_send.at[side, index],
                        g_recv.at[side, index],
                        (target, level),
                    )
    for keep in keeps:
        keep.wait()
    for copy in started:
        copy.wait_send()


def reduce_grads(n_dp, n_shard, grads):
    shard_lines, piece, padded = geometry(n_dp, n_shard)
    half = piece // 2
    count = n_dp.bit_length() - 1
    chunks = 2 * n_shard
    pairs = n_dp // 2
    got_bits = [
        pltpu.VMEM((chunks, pairs >> t, half, LANES), jnp.bfloat16) for t in range(1, count)
    ]
    return pl.pallas_call(
        functools.partial(reduce_kernel, n_dp, n_shard, half),
        out_shape=jax.ShapeDtypeStruct((n_dp, 2, half, LANES), jnp.bfloat16),
        in_specs=[pl.BlockSpec(memory_space=pltpu.HBM)],
        out_specs=pl.BlockSpec(memory_space=pltpu.HBM),
        scratch_shapes=[
            pltpu.VMEM((chunks, pairs, half, LANES), jnp.bfloat16),
            pltpu.VMEM((chunks, pairs, half, LANES), jnp.bfloat16),
            *got_bits,
            pltpu.VMEM((n_shard - 1, 2, half, LANES), jnp.bfloat16),
            pltpu.VMEM((2, half, LANES), jnp.bfloat16),
            pltpu.SemaphoreType.DMA((chunks, pairs)),
            pltpu.SemaphoreType.DMA((chunks, pairs)),
            pltpu.SemaphoreType.DMA((chunks, pairs)),
            pltpu.SemaphoreType.DMA((count - 1, chunks, pairs // 2)),
            pltpu.SemaphoreType.DMA((count - 1, chunks, pairs // 2)),
            pltpu.SemaphoreType.DMA((n_shard - 1, 2)),
            pltpu.SemaphoreType.DMA((n_shard - 1, 2)),
            pltpu.SemaphoreType.DMA((2, n_dp - 1)),
            pltpu.SemaphoreType.DMA((2, n_dp - 1)),
            pltpu.SemaphoreType.DMA((2,)),
        ],
        compiler_params=pltpu.CompilerParams(
            collective_id=2, has_side_effects=True, vmem_limit_bytes=60 << 20
        ),
        name="reduce_grads",
    )(grads.reshape(n_shard, n_dp, 2, half, LANES))


def extended_2(cells, sides, width):
    for axis, dim in sides:
        count = lax.axis_size(axis)
        ends = count - 1
        head = lax.slice_in_dim(cells, 0, width, axis=dim)
        tail = lax.slice_in_dim(cells, cells.shape[dim] - width, cells.shape[dim], axis=dim)
        cells = jnp.concatenate(
            [
                lax.ppermute(tail, axis, [(i, (i + 1) % count) for i in range(ends)]),
                cells,
                lax.ppermute(head, axis, [((i + 1) % count, i) for i in range(ends)]),
            ],
            axis=dim,
        )
    return cells


def gelu_value(preact):
    return 0.5 * preact * (1.0 + lax.erf(preact * sqrt_half))


def gelu_slope(preact):
    return (
        0.5 * (1.0 + lax.erf(preact * sqrt_half))
        + preact * jnp.exp(-0.5 * preact * preact) * inv_root_two_pi
    )


def norm_forward(values, gain_vec, shift_vec):
    centre = jnp.mean(values, axis=-1, keepdims=True)
    centred = values - centre
    spread = jnp.mean(centred * centred, axis=-1, keepdims=True)
    inverse = lax.rsqrt(spread + ln_eps)
    normed = centred * inverse
    return (normed * gain_vec + shift_vec, normed, inverse)


def norm_backward(upstream, normed, inverse, gain_vec):
    scaled = upstream * gain_vec
    first_mean = jnp.mean(scaled, axis=-1, keepdims=True)
    second = jnp.mean(scaled * normed, axis=-1, keepdims=True)
    return inverse * (scaled - first_mean - normed * second)


def split_heads(matrix):
    return matrix.reshape(matrix.shape[0], HEADS, HD)


def block_scores(query_rows, key_rows, allowed):
    raw = jnp.einsum(
        "qhd,khd->hqk",
        split_heads(query_rows),
        split_heads(key_rows),
        preferred_element_type=jnp.float32,
    )
    return jnp.where(allowed[None], raw, masked)


def shards(block_input, cotangent, token_bounds, params, first_moment, second_moment):
    rows_here = block_input.shape[0]
    own_len = params.shape[0]
    n_dp, n_shard = lax.axis_size("dp"), lax.axis_size("shard")
    shard_lines, piece, padded = geometry(n_dp, n_shard)
    own_weights = jnp.pad(params.astype(jnp.bfloat16), (0, padded * LANES - own_len)).reshape(
        n_dp, 2, piece // 2, LANES
    )
    gathered = gather_weights(n_dp, n_shard, own_weights)
    weight_qkv, weight_out, weight_in, weight_back, lines = lay_out_weights(
        n_dp, n_shard, own_weights, gathered
    )
    vector_f = lines[: 8 * D // LANES].reshape(8, D)
    bias_in = lines[8 * D // LANES :].reshape(FF)
    gain_one, shift_one, bias_q, bias_v = (vector_f[0], vector_f[1], vector_f[2], vector_f[3])
    bias_out, gain_two, shift_two, bias_back = (vector_f[4], vector_f[5], vector_f[6], vector_f[7])
    start_tok = token_bounds[0, 0]
    stop_tok = token_bounds[0, 1]
    live_count = stop_tok - start_tok
    slot_ids = jnp.arange(rows_here, dtype=jnp.int32)
    is_live = slot_ids < live_count
    positions = start_tok + slot_ids
    stream = block_input.astype(jnp.float32)
    first_out, first_normed, first_inv = norm_forward(stream, gain_one, shift_one)
    first_feed = first_out.astype(jnp.bfloat16)
    projected = jnp.dot(first_feed, weight_qkv, preferred_element_type=jnp.float32)
    queries = ((projected[:, :D] + bias_q) * 0.125).astype(jnp.bfloat16)
    key_value = jnp.concatenate(
        [projected[:, D : 2 * D], projected[:, 2 * D :] + bias_v], axis=1
    ).astype(jnp.bfloat16)
    rim_rows = jnp.concatenate(
        [key_value[:HALO], lax.dynamic_slice_in_dim(key_value, live_count - HALO, HALO, 0)], axis=0
    )
    rim_pairs = extended_2(rim_rows, ((("dp", "shard"), 0),), HALO)
    spare_rows = KEY_SPAN - BLOCK - 2 * HALO
    extended = jnp.concatenate(
        [
            rim_pairs[:HALO],
            key_value,
            rim_pairs[3 * HALO :],
            jnp.zeros((spare_rows, 2 * D), jnp.bfloat16),
        ],
        axis=0,
    )
    cycle_place = lax.axis_index(("dp", "shard"))
    cycle_last = lax.axis_size(("dp", "shard")) - 1
    lane_ids = jnp.arange(HALO, dtype=jnp.int32)
    key_pos = jnp.concatenate(
        [
            start_tok - HALO + lane_ids,
            positions,
            stop_tok + lane_ids,
            jnp.zeros((spare_rows,), jnp.int32),
        ]
    )
    key_ok = jnp.concatenate(
        [
            jnp.broadcast_to(cycle_place > 0, (HALO,)),
            is_live,
            jnp.broadcast_to(cycle_place < cycle_last, (HALO,)),
            jnp.zeros((spare_rows,), jnp.bool_),
        ]
    )
    key_image = jnp.where(key_ok, key_pos // IMG, -1)
    query_image = positions // IMG

    def block_view(head_row):
        allowed = (
            query_image[head_row : head_row + BLOCK, None]
            == key_image[None, head_row : head_row + KEY_SPAN]
        )
        return (allowed, extended)

    block_num = 0
    head_row = block_num * BLOCK
    allowed, key_part = block_view(head_row)
    scores = block_scores(queries, key_part[:, :D], allowed)
    row_top = jnp.max(scores, axis=-1, keepdims=True)
    log_total = row_top + jnp.log(jnp.sum(jnp.exp(scores - row_top), axis=-1, keepdims=True))
    probs_b = jnp.exp(scores - log_total).astype(jnp.bfloat16)
    block_out = jnp.einsum(
        "hqk,khd->qhd", probs_b, split_heads(key_part[:, D:]), preferred_element_type=jnp.float32
    )
    attended_list = block_out.reshape(BLOCK, D).astype(jnp.bfloat16)
    lse_list = [log_total]
    middle = (
        stream + jnp.dot(attended_list, weight_out, preferred_element_type=jnp.float32) + bias_out
    )
    second_out, second_normed, second_inv = norm_forward(middle, gain_two, shift_two)
    second_feed = second_out.astype(jnp.bfloat16)
    preact = jnp.dot(second_feed, weight_in, preferred_element_type=jnp.float32) + bias_in
    activated = gelu_value(preact).astype(jnp.bfloat16)
    result = (
        middle + jnp.dot(activated, weight_back, preferred_element_type=jnp.float32) + bias_back
    )
    activations = jnp.where(is_live[:, None], result, 0.0)
    tangent_b = jnp.where(is_live[:, None], cotangent, jnp.zeros_like(cotangent))
    tangent = tangent_b.astype(jnp.float32)
    grad_bias_back = jnp.sum(tangent, axis=0)
    slope_in = jnp.einsum(
        "td,fd->tf", tangent_b, weight_back, preferred_element_type=jnp.float32
    ) * gelu_slope(preact)
    grad_bias_in = jnp.sum(slope_in, axis=0)
    slope_feed = slope_in.astype(jnp.bfloat16)
    back_two = jnp.einsum("tf,df->td", slope_feed, weight_in, preferred_element_type=jnp.float32)
    grad_gain_two = jnp.sum(back_two * second_normed, axis=0)
    grad_shift_two = jnp.sum(back_two, axis=0)
    middle_grad = tangent + norm_backward(back_two, second_normed, second_inv, gain_two)
    middle_feed = middle_grad.astype(jnp.bfloat16)
    grad_bias_out = jnp.sum(middle_grad, axis=0)
    attended_grad = jnp.einsum(
        "te,de->td", middle_feed, weight_out, preferred_element_type=jnp.float32
    ).astype(jnp.bfloat16)
    ext_grad = jnp.zeros((rows_here + KEY_SPAN - BLOCK, 2 * D), jnp.float32)
    block_num = 0
    head_row = block_num * BLOCK
    allowed, key_part = block_view(head_row)
    scores = block_scores(queries, key_part[:, :D], allowed)
    probs_f = jnp.exp(scores - lse_list[block_num])
    probs_b = probs_f.astype(jnp.bfloat16)
    grad_part = split_heads(attended_grad)
    value_part = split_heads(key_part[:, D:])
    value_grad = jnp.einsum("hqk,qhd->khd", probs_b, grad_part, preferred_element_type=jnp.float32)
    prob_grad = jnp.einsum(
        "qhd,khd->hqk", grad_part, value_part, preferred_element_type=jnp.float32
    )
    centre_term = jnp.sum(
        grad_part.astype(jnp.float32) * split_heads(attended_list).astype(jnp.float32), axis=-1
    )
    score_grad = (probs_f * (prob_grad - jnp.transpose(centre_term)[:, :, None])).astype(
        jnp.bfloat16
    )
    block_qgrad = jnp.einsum(
        "hqk,khd->qhd", score_grad, split_heads(key_part[:, :D]), preferred_element_type=jnp.float32
    )
    query_grads = block_qgrad.reshape(BLOCK, D) * 0.125
    key_grad = jnp.einsum(
        "hqk,qhd->khd", score_grad, split_heads(queries), preferred_element_type=jnp.float32
    )
    ext_grad = ext_grad.at[head_row : head_row + KEY_SPAN].add(
        jnp.concatenate([key_grad.reshape(KEY_SPAN, D), value_grad.reshape(KEY_SPAN, D)], axis=1)
    )
    outgoing = jnp.concatenate(
        [ext_grad[:HALO], ext_grad[HALO + rows_here : 2 * HALO + rows_here]], axis=0
    )
    incoming = extended_2(outgoing, ((("dp", "shard"), 0),), HALO)
    own_grad = ext_grad[HALO : HALO + rows_here]
    own_grad = own_grad.at[:HALO].add(incoming[:HALO])
    tail_now = lax.dynamic_slice_in_dim(own_grad, live_count - HALO, HALO, 0)
    own_grad = lax.dynamic_update_slice_in_dim(
        own_grad, tail_now + incoming[3 * HALO :], live_count - HALO, 0
    )
    grad_bias_q = jnp.sum(query_grads, axis=0)
    grad_bias_v = jnp.sum(own_grad[:, D:], axis=0)
    joined = jnp.concatenate([query_grads, own_grad], axis=1).astype(jnp.bfloat16)
    back_one = jnp.einsum("te,de->td", joined, weight_qkv, preferred_element_type=jnp.float32)
    grad_gain_one = jnp.sum(back_one * first_normed, axis=0)
    grad_shift_one = jnp.sum(back_one, axis=0)
    stream_grad = middle_grad + norm_backward(back_one, first_normed, first_inv, gain_one)
    input_grad = jnp.where(is_live[:, None], stream_grad, 0.0)
    vector_grad = jnp.stack(
        [
            grad_gain_one,
            grad_shift_one,
            grad_bias_q,
            grad_bias_v,
            grad_bias_out,
            grad_gain_two,
            grad_shift_two,
            grad_bias_back,
        ]
    )
    vector_lines = jnp.concatenate([vector_grad.reshape(-1), grad_bias_in]).reshape(-1, LANES)
    flat_grads = weight_grads(
        n_dp,
        n_shard,
        first_feed,
        joined,
        attended_list,
        middle_feed,
        second_feed,
        slope_feed,
        activated,
        tangent_b,
        vector_lines,
    )
    reduced = reduce_grads(n_dp, n_shard, flat_grads).reshape(-1)
    piece_len = own_len // n_dp
    grad_shard = reduced[:own_len].astype(jnp.float32)
    grad_piece = lax.dynamic_slice_in_dim(
        grad_shard, lax.axis_index("dp") * piece_len, piece_len, 0
    )
    matrices = 4 * D * D + 2 * D * FF
    global_ids = lax.axis_index("shard") * own_len + jnp.arange(own_len, dtype=jnp.int32)
    decays = (global_ids < matrices).astype(jnp.float32)
    new_first = beta_one * first_moment + (1.0 - beta_one) * grad_shard
    new_second = beta_two * second_moment + (1.0 - beta_two) * grad_shard * grad_shard
    first_hat = new_first / (1.0 - beta_one**3)
    second_hat = new_second / (1.0 - beta_two**3)
    new_params = params - learn_rate * (
        first_hat / (jnp.sqrt(second_hat) + adam_eps) + decay_rate * decays * params
    )
    param_grad = grad_piece.reshape(1, 1, piece_len)
    return (activations, input_grad, param_grad, new_params, new_first, new_second)


def solution(mesh):
    in_specs = (
        P(("dp", "shard"), None),
        P(("dp", "shard"), None),
        P(("dp", "shard"), None),
        P("shard"),
        P("shard"),
        P("shard"),
    )
    out_specs = (
        P(("dp", "shard"), None),
        P(("dp", "shard"), None),
        P("shard", "dp", None),
        P("shard"),
        P("shard"),
        P("shard"),
    )
    return jax.shard_map(shards, mesh=mesh, in_specs=in_specs, out_specs=out_specs, check_vma=False)
```

```python
import functools

import jax
import jax.numpy as jnp
from jax import lax
from jax.experimental import pallas as pl
from jax.experimental.pallas import tpu as pltpu
from jax.sharding import PartitionSpec as P

D = 768
HEADS = 12
HD = 64
FF = 3072
IMG = 197
BLOCK = 512


ln_eps = 1e-06
masked = -1e30
beta_one = 0.9
beta_two = 0.999
learn_rate = 0.02
decay_rate = 0.05
adam_eps = 1e-08
sqrt_half = 0.7071067811865476
inv_root_two_pi = 0.3989422804014327


MESH = pl.DeviceIdType.MESH
LANES = 128
MARGIN = 64


def geometry(n_dp, n_shard):
    total = 4 * D * D + 2 * D * FF + 8 * D + FF
    shard_lines = total // n_shard // LANES
    piece = -(-shard_lines // n_dp // 32) * 32
    piece = -(-(-(-shard_lines // n_dp)) // 32) * 32
    return shard_lines, piece, piece * n_dp


def bit_list(n_dp):
    count = n_dp.bit_length() - 1
    return count, [list(range(1, count)), list(range(count - 1, 0, -1))]


def bits_of(index, count):
    return [lax.rem(lax.div(index, 1 << b), 2) for b in range(count)]


def flipped(index, bits, which):
    return index + sum((1 << b) * (1 - 2 * bits[b]) for b in which)


def greet(n_dp, n_shard, place, level, bits, extra=()):
    barrier = pltpu.get_barrier_semaphore()
    peers = [(place, lax.rem(level + j, n_shard)) for j in range(1, n_shard)]
    peers += [(flipped(place, bits, [b]), level) for b in range(len(bits))]
    peers += list(extra)
    for peer in peers:
        pl.semaphore_signal(barrier, inc=1, device_id=peer, device_id_type=MESH)
    pl.semaphore_wait(barrier, len(peers))


def subsets(order):
    found = [[]]
    for b in order:
        found = found + [kept + [b] for kept in found]
    return found


def ring(n_dp, n_shard, place, level):
    spot = place * n_shard + level
    size = n_dp * n_shard
    sides = [lax.rem(spot + size - 1, size), lax.rem(spot + 1, size)]
    return [(lax.div(side, n_shard), lax.rem(side, n_shard)) for side in sides]


def gather_kernel(
    n_dp, n_shard, half, own, head, tail, out, before, after, z_send, z_recv, d_send, d_recv, r_send, r_recv
):
    place = lax.axis_index("dp")
    level = lax.axis_index("shard")
    count, orders = bit_list(n_dp)
    bits = bits_of(place, count)
    previous, following = ring(n_dp, n_shard, place, level)
    greet(n_dp, n_shard, place, level, bits, (previous, following))
    started = []

    def push(src, dst, send, recv, target):
        copy = pltpu.make_async_remote_copy(
            src_ref=src,
            dst_ref=dst,
            send_sem=send,
            recv_sem=recv,
            device_id=target,
            device_id_type=MESH,
        )
        copy.start()
        started.append(copy)

    push(head, after, r_send.at[0], r_recv.at[0], previous)
    push(tail, before, r_send.at[1], r_recv.at[1], following)
    for side in range(2):
        for j in range(1, n_shard):
            push(
                own.at[place, side],
                out.at[level, place, side],
                z_send.at[j - 1, side],
                z_recv.at[j - 1, side],
                (place, lax.rem(level + j, n_shard)),
            )
    chunks = [(j, side) for j in range(1, n_shard) for side in range(2)]

    def advance(chunk, stage):
        j, side = chunks[chunk]
        source = lax.rem(level - j + n_shard, n_shard)
        order = orders[side] + [0]

        def arrived(piece, sem):
            pltpu.make_async_remote_copy(
                src_ref=own.at[place, side],
                dst_ref=out.at[source, piece, side],
                send_sem=z_send.at[0, 0],
                recv_sem=sem,
                device_id=(place, level),
                device_id_type=MESH,
            ).wait_recv()

        if stage == 0:
            arrived(place, z_recv.at[j - 1, side])
        else:
            partner = flipped(place, bits, [order[stage - 1]])
            for slot, which in enumerate(subsets(order[: stage - 1])):
                arrived(
                    flipped(place, bits, which + [order[stage - 1]]),
                    d_recv.at[chunk, (1 << (stage - 1)) - 1 + slot],
                )
        if stage < count:
            partner = flipped(place, bits, [order[stage]])
            for slot, which in enumerate(subsets(order[:stage])):
                piece = flipped(place, bits, which)
                index = (1 << stage) - 1 + slot
                push(
                    out.at[source, piece, side],
                    out.at[source, piece, side],
                    d_send.at[chunk, index],
                    d_recv.at[chunk, index],
                    (partner, level),
                )

    for tick in range(len(chunks) + count):
        for stage in range(count + 1):
            chunk = tick - stage
            if 0 <= chunk < len(chunks):
                advance(chunk, stage)
    started[0].wait_recv()
    started[1].wait_recv()
    for copy in started:
        copy.wait_send()


def gather_weights(n_dp, n_shard, own, head, tail):
    shard_lines, piece, padded = geometry(n_dp, n_shard)
    half = piece // 2
    chunks = 2 * (n_shard - 1)
    space = pl.BlockSpec(memory_space=pltpu.HBM)
    return pl.pallas_call(
        functools.partial(gather_kernel, n_dp, n_shard, half),
        out_shape=[
            jax.ShapeDtypeStruct((n_shard, n_dp, 2, half, LANES), jnp.bfloat16),
            jax.ShapeDtypeStruct((RIM, D), jnp.bfloat16),
            jax.ShapeDtypeStruct((RIM, D), jnp.bfloat16),
        ],
        in_specs=[space] * 3,
        out_specs=[space] * 3,
        scratch_shapes=[
            pltpu.SemaphoreType.DMA((n_shard - 1, 2)),
            pltpu.SemaphoreType.DMA((n_shard - 1, 2)),
            pltpu.SemaphoreType.DMA((chunks, n_dp - 1)),
            pltpu.SemaphoreType.DMA((chunks, n_dp - 1)),
            pltpu.SemaphoreType.DMA((2,)),
            pltpu.SemaphoreType.DMA((2,)),
        ],
        compiler_params=pltpu.CompilerParams(collective_id=1, has_side_effects=True),
        name="gather_weights",
    )(own, head, tail)


def weight_plan(n_shard, shard_lines):
    sizes = [(D, 3 * D), (D, D), (D, FF), (FF, D)]
    plan = [[] for _ in range(n_shard)]
    cursor = 0
    for which, (rows, columns) in enumerate(sizes):
        width = columns // LANES
        first = 0
        for s in range(n_shard):
            stop = (s + 1) * shard_lines
            last = min(rows, max(first, (stop - cursor) // width))
            last = last if last == rows else last // 128 * 128
            if last > first:
                plan[s].append((which, first, last, width, cursor + first * width - s * shard_lines))
                first = last
        cursor += rows * width
    return plan, cursor


def layout_kernel(n_shard, shard_lines, padded, own, got, wqkv, wout, win, wback, vec, raw, wide, sem):
    level = lax.axis_index("shard")
    plan, tail = weight_plan(n_shard, shard_lines)
    targets = [wqkv, wout, win, wback]

    def load(s, slot):
        @pl.when(level == s)
        def _():
            pltpu.make_async_copy(own, raw.at[slot], sem.at[slot]).start()

        @pl.when(level != s)
        def _():
            pltpu.make_async_copy(got.at[s], raw.at[slot], sem.at[slot]).start()

    load(0, 0)
    for s in range(n_shard):
        slot = s % 2
        pltpu.make_async_copy(own, raw.at[slot], sem.at[slot]).wait()
        if s + 1 < n_shard:
            load(s + 1, 1 - slot)
        if s:
            wide[0:MARGIN, :] = wide[shard_lines : shard_lines + MARGIN, :]

        def spread(i, carry):
            at = pl.multiple_of(i * 128, 128)
            wide[pl.ds(MARGIN + at, 128), :] = raw[slot, pl.ds(at, 128), :].astype(jnp.float32)
            return carry

        lax.fori_loop(0, padded // 128, spread, 0)
        for which, first, last, width, offset in plan[s]:
            target = targets[which]

            def rows(i, carry):
                at = pl.multiple_of(first + i * 16, 16)
                line = MARGIN + offset + i * (16 * width)
                for c in range(width):
                    target[pl.ds(at, 16), c * LANES : (c + 1) * LANES] = wide[
                        pl.ds(line + c, 16, stride=width), :
                    ].astype(jnp.bfloat16)
                return carry

            lax.fori_loop(0, (last - first) // 16, rows, 0)
    start = MARGIN + tail - (n_shard - 1) * shard_lines
    vec[...] = wide[start : start + vec.shape[0], :]


def lay_out_weights(n_dp, n_shard, own, got):
    shard_lines, piece, padded = geometry(n_dp, n_shard)
    count = (8 * D + FF) // LANES
    shapes = [(D, 3 * D), (D, D), (D, FF), (FF, D)]
    return pl.pallas_call(
        functools.partial(layout_kernel, n_shard, shard_lines, padded),
        out_shape=[jax.ShapeDtypeStruct(shape, jnp.bfloat16) for shape in shapes]
        + [jax.ShapeDtypeStruct((count, LANES), jnp.float32)],
        in_specs=[pl.BlockSpec(memory_space=pltpu.HBM)] * 2,
        out_specs=[pl.BlockSpec(memory_space=pltpu.VMEM)] * 5,
        scratch_shapes=[
            pltpu.VMEM((2, padded, LANES), jnp.bfloat16),
            pltpu.VMEM((MARGIN + padded, LANES), jnp.float32),
            pltpu.SemaphoreType.DMA((2,)),
        ],
        compiler_params=pltpu.CompilerParams(vmem_limit_bytes=60 << 20),
        name="lay_out_weights",
    )(own.reshape(padded, LANES), got.reshape(n_shard, padded, LANES))


def weight_grad_kernel(
    n_shard, shard_lines, padded, feed_one, joined, attended, middle, feed_two, slope, activated, tangent, vec, out, wide, narrow, sem
):
    lefts = [feed_one, attended, feed_two, activated]
    rights = [joined, middle, slope, tangent]
    sizes = [(D, 3 * D), (D, D), (D, FF), (FF, D)]
    cursor = 0
    plan = [[] for _ in range(n_shard)]
    for which, (rows, columns) in enumerate(sizes):
        width = columns // LANES
        for s in range(n_shard):
            begin, stop = s * shard_lines, (s + 1) * shard_lines
            first = max(0, (begin - cursor) // width)
            last = min(rows, -(-(stop - cursor) // width))
            if last > first:
                first = first // 128 * 128
                plan[s].append((which, first, last, width, cursor - begin))
        cursor += rows * width
    tail = cursor - (n_shard - 1) * shard_lines

    def product(which, row, width, group):
        return lax.dot_general(
            lefts[which][:, pl.ds(row, 128)],
            rights[which][:, group * 768 : (group + 1) * 768],
            (((0,), (0,)), ((), ())),
            preferred_element_type=jnp.float32,
        )

    for s in range(n_shard):
        for which, first, last, width, offset in plan[s]:
            full = (last - first) // 128

            def block(i, carry):
                row = pl.multiple_of(first + i * 128, 128)
                line = MARGIN + offset + row * width
                for group in range(width // 6):
                    tile = product(which, row, width, group)
                    for c in range(6):
                        wide[pl.ds(line + group * 6 + c, 128, stride=width), :] = tile[
                            :, c * LANES : (c + 1) * LANES
                        ]
                return carry

            if full:
                lax.fori_loop(0, full, block, 0)
            row = first + full * 128
            rest = -(-(last - row) // 8) * 8
            if rest:
                line = MARGIN + offset + row * width
                for group in range(width // 6):
                    tile = product(which, row, width, group)
                    for c in range(6):
                        wide[pl.ds(line + group * 6 + c, rest, stride=width), :] = tile[
                            :rest, c * LANES : (c + 1) * LANES
                        ]
        if s == n_shard - 1:
            wide[MARGIN + tail : MARGIN + tail + vec.shape[0], :] = vec[...]
        slot = s % 2
        if s >= 2:
            pltpu.make_async_copy(narrow.at[slot], out.at[s - 2], sem.at[slot]).wait()

        def pack(i, carry):
            at = pl.multiple_of(i * 128, 128)
            narrow[slot, pl.ds(at, 128), :] = wide[pl.ds(MARGIN + at, 128), :].astype(jnp.bfloat16)
            return carry

        lax.fori_loop(0, padded // 128, pack, 0)
        pltpu.make_async_copy(narrow.at[slot], out.at[s], sem.at[slot]).start()
    for s in range(n_shard - 2, n_shard):
        pltpu.make_async_copy(narrow.at[s % 2], out.at[s], sem.at[s % 2]).wait()


def weight_grads(n_dp, n_shard, *operands):
    shard_lines, piece, padded = geometry(n_dp, n_shard)
    return pl.pallas_call(
        functools.partial(weight_grad_kernel, n_shard, shard_lines, padded),
        out_shape=jax.ShapeDtypeStruct((n_shard, padded, LANES), jnp.bfloat16),
        in_specs=[pl.BlockSpec(memory_space=pltpu.VMEM)] * 9,
        out_specs=pl.BlockSpec(memory_space=pltpu.HBM),
        scratch_shapes=[
            pltpu.VMEM((MARGIN + padded + 128, LANES), jnp.float32),
            pltpu.VMEM((2, padded, LANES), jnp.bfloat16),
            pltpu.SemaphoreType.DMA((2,)),
        ],
        compiler_params=pltpu.CompilerParams(vmem_limit_bytes=60 << 20),
        name="weight_grads",
    )(*operands)


def reduce_kernel(n_dp, n_shard, half, grads, out, *scratch):
    count, orders = bit_list(n_dp)
    acc, got_core = scratch[0], scratch[1]
    got_bits = scratch[2 : 1 + count]
    got_z, final = scratch[1 + count : 3 + count]
    load_sem, core_send, core_recv, bit_send, bit_recv, z_send, z_recv, g_send, g_recv, keep_sem = scratch[
        3 + count :
    ]
    place = lax.axis_index("dp")
    level = lax.axis_index("shard")
    bits = bits_of(place, count)
    pairs = n_dp // 2
    chunks = [(j, side) for j in list(range(1, n_shard)) + [0] for side in range(2)]
    step = 176 if half % 176 == 0 else 32
    greet(n_dp, n_shard, place, level, bits)
    started = []

    def push(src, dst, send, recv, target):
        copy = pltpu.make_async_remote_copy(
            src_ref=src,
            dst_ref=dst,
            send_sem=send,
            recv_sem=recv,
            device_id=target,
            device_id_type=MESH,
        )
        copy.start()
        started.append(copy)

    def landed(buffer, sem):
        pltpu.make_async_remote_copy(
            src_ref=buffer,
            dst_ref=buffer,
            send_sem=z_send.at[0, 0],
            recv_sem=sem,
            device_id=(place, level),
            device_id_type=MESH,
        ).wait_recv()

    core = bits[0]
    partner = flipped(place, bits, [0])
    for chunk, (j, side) in enumerate(chunks):
        target = lax.rem(level + j, n_shard)
        for m in range(pairs):
            push(
                grads.at[target, 2 * m + 1 - core, side],
                got_core.at[chunk, m],
                core_send.at[chunk, m],
                core_recv.at[chunk, m],
                (partner, level),
            )
            pltpu.make_async_copy(
                grads.at[target, 2 * m + core, side], acc.at[chunk, m], load_sem.at[chunk, m]
            ).start()

    def add(into, other):
        def body(i, carry):
            at = pl.multiple_of(i * step, 16)
            total = into[pl.ds(at, step), :].astype(jnp.float32) + other[pl.ds(at, step), :].astype(
                jnp.float32
            )
            into[pl.ds(at, step), :] = total.astype(jnp.bfloat16)
            return carry

        lax.fori_loop(0, half // step, body, 0)

    def members(order, stage, flip):
        fixed = order[:stage]
        base = sum((bits[b] if b != flip else 1 - bits[b]) * (1 << (b - 1)) for b in fixed)
        return [base + sum(1 << (b - 1) for b in which) for which in subsets(order[stage:])]

    def advance(chunk, stage):
        j, side = chunks[chunk]
        order = orders[side]
        if stage == 0:
            for m in range(pairs):
                pltpu.make_async_copy(
                    grads.at[0, 2 * m + core, side], acc.at[chunk, m], load_sem.at[chunk, m]
                ).wait()
                landed(got_core.at[chunk, m], core_recv.at[chunk, m])
                add(acc.at[chunk, m], got_core.at[chunk, m])
        else:
            for slot, m in enumerate(members(order, stage, None)):
                buffer = got_bits[stage - 1].at[chunk, slot]
                landed(buffer, bit_recv.at[stage - 1, chunk, slot])
                add(acc.at[chunk, m], buffer)
        if stage < count - 1:
            flip = order[stage]
            target = flipped(place, bits, [flip])
            for slot, m in enumerate(members(order, stage + 1, flip)):
                push(
                    acc.at[chunk, m],
                    got_bits[stage].at[chunk, slot],
                    bit_send.at[stage, chunk, slot],
                    bit_recv.at[stage, chunk, slot],
                    (target, level),
                )
        elif j:
            (m,) = members(order, stage, None)
            push(
                acc.at[chunk, m],
                got_z.at[j - 1, side],
                z_send.at[j - 1, side],
                z_recv.at[j - 1, side],
                (place, lax.rem(level + j, n_shard)),
            )

    for tick in range(len(chunks) + count - 1):
        for stage in range(count):
            chunk = tick - stage
            if 0 <= chunk < len(chunks):
                advance(chunk, stage)

    mine = sum(bits[b] * (1 << (b - 1)) for b in range(1, count))
    keeps = []
    for side in range(2):
        chunk = chunks.index((0, side))
        for j in range(1, n_shard):
            landed(got_z.at[j - 1, side], z_recv.at[j - 1, side])

        def body(i, carry):
            at = pl.multiple_of(i * step, 16)
            total = acc[chunk, mine, pl.ds(at, step), :].astype(jnp.float32)
            for j in range(1, n_shard):
                total = total + got_z[j - 1, side, pl.ds(at, step), :].astype(jnp.float32)
            final[side, pl.ds(at, step), :] = total.astype(jnp.bfloat16)
            return carry

        lax.fori_loop(0, half // step, body, 0)
        keep = pltpu.make_async_copy(final.at[side], out.at[place, side], keep_sem.at[side])
        keep.start()
        keeps.append(keep)
        push(
            final.at[side],
            out.at[place, side],
            g_send.at[side, 0],
            g_recv.at[side, 0],
            (flipped(place, bits, [orders[side][0]]), level),
        )
    for stage in range(1, count + 1):
        for side in range(2):
            order = orders[side] + [0]
            for slot, which in enumerate(subsets(order[: stage - 1])):
                landed(
                    out.at[flipped(place, bits, which + [order[stage - 1]]), side],
                    g_recv.at[side, (1 << (stage - 1)) - 1 + slot],
                )
            if stage < count:
                target = flipped(place, bits, [order[stage]])
                for slot, which in enumerate(subsets(order[:stage])):
                    piece = flipped(place, bits, which)
                    index = (1 << stage) - 1 + slot
                    push(
                        final.at[side] if not which else out.at[piece, side],
                        out.at[piece, side],
                        g_send.at[side, index],
                        g_recv.at[side, index],
                        (target, level),
                    )
    for keep in keeps:
        keep.wait()
    for copy in started:
        copy.wait_send()


def reduce_grads(n_dp, n_shard, grads):
    shard_lines, piece, padded = geometry(n_dp, n_shard)
    half = piece // 2
    count = n_dp.bit_length() - 1
    chunks = 2 * n_shard
    pairs = n_dp // 2
    got_bits = [
        pltpu.VMEM((chunks, pairs >> t, half, LANES), jnp.bfloat16) for t in range(1, count)
    ]
    return pl.pallas_call(
        functools.partial(reduce_kernel, n_dp, n_shard, half),
        out_shape=jax.ShapeDtypeStruct((n_dp, 2, half, LANES), jnp.bfloat16),
        in_specs=[pl.BlockSpec(memory_space=pltpu.HBM)],
        out_specs=pl.BlockSpec(memory_space=pltpu.HBM),
        scratch_shapes=[
            pltpu.VMEM((chunks, pairs, half, LANES), jnp.bfloat16),
            pltpu.VMEM((chunks, pairs, half, LANES), jnp.bfloat16),
            *got_bits,
            pltpu.VMEM((n_shard - 1, 2, half, LANES), jnp.bfloat16),
            pltpu.VMEM((2, half, LANES), jnp.bfloat16),
            pltpu.SemaphoreType.DMA((chunks, pairs)),
            pltpu.SemaphoreType.DMA((chunks, pairs)),
            pltpu.SemaphoreType.DMA((chunks, pairs)),
            pltpu.SemaphoreType.DMA((count - 1, chunks, pairs // 2)),
            pltpu.SemaphoreType.DMA((count - 1, chunks, pairs // 2)),
            pltpu.SemaphoreType.DMA((n_shard - 1, 2)),
            pltpu.SemaphoreType.DMA((n_shard - 1, 2)),
            pltpu.SemaphoreType.DMA((2, n_dp - 1)),
            pltpu.SemaphoreType.DMA((2, n_dp - 1)),
            pltpu.SemaphoreType.DMA((2,)),
        ],
        compiler_params=pltpu.CompilerParams(
            collective_id=2, has_side_effects=True, vmem_limit_bytes=60 << 20
        ),
        name="reduce_grads",
    )(grads.reshape(n_shard, n_dp, 2, half, LANES))


RIM = 208
EXT = 1024
QB = 128
WIN = 640


def window_bias(start, block):
    inv = 1.0 / IMG
    rows = lax.broadcasted_iota(jnp.int32, (QB, 1), 0) + (start + block * QB)
    cols = lax.broadcasted_iota(jnp.int32, (1, WIN), 1) + (start - RIM + block * QB)
    row_image = jnp.floor((rows.astype(jnp.float32) + 0.5) * inv)
    col_image = jnp.floor((cols.astype(jnp.float32) + 0.5) * inv)
    return jnp.where(row_image == col_image, 0.0, masked)


def stacked(rows):
    lane = lax.broadcasted_iota(jnp.int32, (QB, LANES), 1)
    zero = jnp.zeros_like(rows)
    return jnp.concatenate([jnp.where(lane < HD, rows, zero), jnp.where(lane < HD, zero, rows)], axis=0)


def unstacked(rows):
    lane = lax.broadcasted_iota(jnp.int32, (QB, LANES), 1)
    return jnp.where(lane < HD, rows[:QB], rows[QB:])


def attend_kernel(bounds, rows, weight, vectors, feed, queries, keys, values, attended, lse, wide_feed, bias):
    start = bounds[0, 0]
    gain, shift = vectors[0:1, :], vectors[1:2, :]

    def norm(i, carry):
        at = pl.multiple_of(i * 64, 64)
        x = rows[pl.ds(at, 64), :].astype(jnp.float32)
        centred = x - jnp.mean(x, axis=-1, keepdims=True)
        inverse = lax.rsqrt(jnp.mean(centred * centred, axis=-1, keepdims=True) + ln_eps)
        wide_feed[pl.ds(at, 64), :] = (centred * inverse * gain + shift).astype(jnp.bfloat16)
        return carry

    lax.fori_loop(0, EXT // 64, norm, 0)
    feed[...] = wide_feed[RIM : RIM + BLOCK, :]

    def project(i, carry):
        at = pl.multiple_of(i * 256, 256)
        block = wide_feed[pl.ds(at, 256), :]
        keys[pl.ds(at, 256), :] = jnp.dot(
            block, weight[:, D : 2 * D], preferred_element_type=jnp.float32
        ).astype(jnp.bfloat16)
        values[pl.ds(at, 256), :] = (
            jnp.dot(block, weight[:, 2 * D :], preferred_element_type=jnp.float32) + vectors[3:4, :]
        ).astype(jnp.bfloat16)
        return carry

    lax.fori_loop(0, EXT // 256, project, 0)

    def ask(i, carry):
        at = pl.multiple_of(i * 256, 256)
        queries[pl.ds(at, 256), :] = (
            (jnp.dot(feed[pl.ds(at, 256), :], weight[:, :D], preferred_element_type=jnp.float32) + vectors[2:3, :])
            * 0.125
        ).astype(jnp.bfloat16)
        return carry

    lax.fori_loop(0, BLOCK // 256, ask, 0)
    for block in range(BLOCK // QB):
        bias[block] = window_bias(start, block)

    def attend(i, carry):
        block = lax.rem(i, BLOCK // QB)
        pair = lax.div(i, BLOCK // QB)
        at = pl.multiple_of(block * QB, QB)
        lanes = pl.ds(pl.multiple_of(pair * LANES, LANES), LANES)
        scores = lax.dot_general(
            stacked(queries[pl.ds(at, QB), lanes]),
            keys[pl.ds(at, WIN), lanes],
            (((1,), (1,)), ((), ())),
            preferred_element_type=jnp.float32,
        )
        cover = bias[block]
        scores = scores + jnp.concatenate([cover, cover], axis=0)
        top = jnp.max(scores, axis=-1, keepdims=True)
        raised = jnp.exp(scores - top)
        total = jnp.sum(raised, axis=-1, keepdims=True)
        probs = (raised * (1.0 / total)).astype(jnp.bfloat16)
        out = jnp.dot(probs, values[pl.ds(at, WIN), lanes], preferred_element_type=jnp.float32)
        attended[pl.ds(at, QB), lanes] = unstacked(out).astype(jnp.bfloat16)
        lse[pair, block] = jnp.broadcast_to(top + jnp.log(total), (2 * QB, LANES))
        return carry

    lax.fori_loop(0, HEADS // 2 * (BLOCK // QB), attend, 0)


def attend(bounds, rows, weight, vectors):
    half = jnp.bfloat16
    return pl.pallas_call(
        attend_kernel,
        out_shape=[
            jax.ShapeDtypeStruct((BLOCK, D), half),
            jax.ShapeDtypeStruct((BLOCK, D), half),
            jax.ShapeDtypeStruct((EXT, D), half),
            jax.ShapeDtypeStruct((EXT, D), half),
            jax.ShapeDtypeStruct((BLOCK, D), half),
            jax.ShapeDtypeStruct((HEADS // 2, BLOCK // QB, 2 * QB, LANES), jnp.float32),
        ],
        in_specs=[pl.BlockSpec(memory_space=pltpu.SMEM)] + [pl.BlockSpec(memory_space=pltpu.VMEM)] * 3,
        out_specs=[pl.BlockSpec(memory_space=pltpu.VMEM)] * 6,
        scratch_shapes=[
            pltpu.VMEM((EXT, D), half),
            pltpu.VMEM((BLOCK // QB, QB, WIN), jnp.float32),
        ],
        compiler_params=pltpu.CompilerParams(vmem_limit_bytes=60 << 20),
        name="attend",
    )(bounds, rows, weight, vectors)


def attend_back_kernel(bounds, queries, keys, values, attended, grads, lse, query_grad, key_grad, value_grad, bias):
    start = bounds[0, 0]
    for block in range(BLOCK // QB):
        bias[block] = window_bias(start, block)
    key_grad[...] = jnp.zeros_like(key_grad)
    value_grad[...] = jnp.zeros_like(value_grad)

    def body(i, carry):
        block = lax.rem(i, BLOCK // QB)
        pair = lax.div(i, BLOCK // QB)
        at = pl.multiple_of(block * QB, QB)
        lanes = pl.ds(pl.multiple_of(pair * LANES, LANES), LANES)
        asked = stacked(queries[pl.ds(at, QB), lanes])
        own_grad = grads[pl.ds(at, QB), lanes]
        given = stacked(own_grad)
        near_keys = keys[pl.ds(at, WIN), lanes]
        near_values = values[pl.ds(at, WIN), lanes]
        scores = lax.dot_general(
            asked, near_keys, (((1,), (1,)), ((), ())), preferred_element_type=jnp.float32
        )
        cover = bias[block]
        level = lse[pair, block]
        probs = jnp.exp(
            scores + jnp.concatenate([cover, cover], axis=0) - jnp.concatenate([level] * (WIN // LANES), axis=1)
        )
        prob_grad = lax.dot_general(
            given, near_values, (((1,), (1,)), ((), ())), preferred_element_type=jnp.float32
        )
        wide = given.astype(jnp.float32) * jnp.concatenate([attended[pl.ds(at, QB), lanes]] * 2, axis=0).astype(
            jnp.float32
        )
        centre = jnp.sum(wide, axis=-1, keepdims=True)
        score_grad = (probs * (prob_grad - centre)).astype(jnp.bfloat16)
        query_grad[pl.ds(at, QB), lanes] = (
            unstacked(jnp.dot(score_grad, near_keys, preferred_element_type=jnp.float32)) * 0.125
        )
        key_grad[pl.ds(at, WIN), lanes] += lax.dot_general(
            score_grad, asked, (((0,), (0,)), ((), ())), preferred_element_type=jnp.float32
        )
        value_grad[pl.ds(at, WIN), lanes] += lax.dot_general(
            probs.astype(jnp.bfloat16), given, (((0,), (0,)), ((), ())), preferred_element_type=jnp.float32
        )
        return carry

    lax.fori_loop(0, HEADS // 2 * (BLOCK // QB), body, 0)


def attend_back(bounds, queries, keys, values, attended, grads, lse):
    return pl.pallas_call(
        attend_back_kernel,
        out_shape=[
            jax.ShapeDtypeStruct((BLOCK, D), jnp.float32),
            jax.ShapeDtypeStruct((EXT, D), jnp.float32),
            jax.ShapeDtypeStruct((EXT, D), jnp.float32),
        ],
        in_specs=[pl.BlockSpec(memory_space=pltpu.SMEM)] + [pl.BlockSpec(memory_space=pltpu.VMEM)] * 6,
        out_specs=[pl.BlockSpec(memory_space=pltpu.VMEM)] * 3,
        scratch_shapes=[pltpu.VMEM((BLOCK // QB, QB, WIN), jnp.float32)],
        compiler_params=pltpu.CompilerParams(vmem_limit_bytes=60 << 20),
        name="attend_back",
    )(bounds, queries, keys, values, attended, grads, lse)


def gelu_value(preact):
    return 0.5 * preact * (1.0 + lax.erf(preact * sqrt_half))


def gelu_slope(preact):
    return (
        0.5 * (1.0 + lax.erf(preact * sqrt_half))
        + preact * jnp.exp(-0.5 * preact * preact) * inv_root_two_pi
    )


def norm_stats(values):
    centred = values - jnp.mean(values, axis=-1, keepdims=True)
    inverse = lax.rsqrt(jnp.mean(centred * centred, axis=-1, keepdims=True) + ln_eps)
    return centred * inverse, inverse


def norm_forward(values, gain_vec, shift_vec):
    centre = jnp.mean(values, axis=-1, keepdims=True)
    centred = values - centre
    spread = jnp.mean(centred * centred, axis=-1, keepdims=True)
    inverse = lax.rsqrt(spread + ln_eps)
    normed = centred * inverse
    return (normed * gain_vec + shift_vec, normed, inverse)


def norm_backward(upstream, normed, inverse, gain_vec):
    scaled = upstream * gain_vec
    first_mean = jnp.mean(scaled, axis=-1, keepdims=True)
    second = jnp.mean(scaled * normed, axis=-1, keepdims=True)
    return inverse * (scaled - first_mean - normed * second)


def shards(block_input, cotangent, token_bounds, params, first_moment, second_moment):
    rows_here = block_input.shape[0]
    own_len = params.shape[0]
    n_dp, n_shard = lax.axis_size("dp"), lax.axis_size("shard")
    shard_lines, piece, padded = geometry(n_dp, n_shard)
    own_weights = jnp.pad(params.astype(jnp.bfloat16), (0, padded * LANES - own_len)).reshape(
        n_dp, 2, piece // 2, LANES
    )
    live_count = token_bounds[0, 1] - token_bounds[0, 0]
    tail_rows = lax.dynamic_slice_in_dim(jnp.pad(block_input, ((16, 0), (0, 0))), live_count + (16 - RIM), RIM, 0)
    gathered, before, after = gather_weights(n_dp, n_shard, own_weights, block_input[:RIM], tail_rows)
    weight_qkv, weight_out, weight_in, weight_back, lines = lay_out_weights(
        n_dp, n_shard, own_weights, gathered
    )
    vector_f = lines[: 8 * D // LANES].reshape(8, D)
    bias_in = lines[8 * D // LANES :].reshape(FF)
    gain_one, shift_one, bias_q, bias_v = (vector_f[0], vector_f[1], vector_f[2], vector_f[3])
    bias_out, gain_two, shift_two, bias_back = (vector_f[4], vector_f[5], vector_f[6], vector_f[7])
    slot_ids = jnp.arange(rows_here, dtype=jnp.int32)
    is_live = slot_ids < live_count
    stream = block_input.astype(jnp.float32)
    first_normed, first_inv = norm_stats(stream)
    wide_rows = jnp.concatenate(
        [before, block_input, jnp.zeros((EXT - RIM - BLOCK, D), jnp.bfloat16)], axis=0
    )
    wide_rows = lax.dynamic_update_slice_in_dim(wide_rows, after, RIM + live_count, 0)
    first_feed, queries, keys, values, attended_list, lse = attend(
        token_bounds, wide_rows, weight_qkv, vector_f
    )
    middle = (
        stream + jnp.dot(attended_list, weight_out, preferred_element_type=jnp.float32) + bias_out
    )
    second_out, second_normed, second_inv = norm_forward(middle, gain_two, shift_two)
    second_feed = second_out.astype(jnp.bfloat16)
    preact = jnp.dot(second_feed, weight_in, preferred_element_type=jnp.float32) + bias_in
    activated = gelu_value(preact).astype(jnp.bfloat16)
    result = (
        middle + jnp.dot(activated, weight_back, preferred_element_type=jnp.float32) + bias_back
    )
    activations = jnp.where(is_live[:, None], result, 0.0)
    tangent_b = jnp.where(is_live[:, None], cotangent, jnp.zeros_like(cotangent))
    tangent = tangent_b.astype(jnp.float32)
    grad_bias_back = jnp.sum(tangent, axis=0)
    slope_in = jnp.einsum(
        "td,fd->tf", tangent_b, weight_back, preferred_element_type=jnp.float32
    ) * gelu_slope(preact)
    grad_bias_in = jnp.sum(slope_in, axis=0)
    slope_feed = slope_in.astype(jnp.bfloat16)
    back_two = jnp.einsum("tf,df->td", slope_feed, weight_in, preferred_element_type=jnp.float32)
    grad_gain_two = jnp.sum(back_two * second_normed, axis=0)
    grad_shift_two = jnp.sum(back_two, axis=0)
    middle_grad = tangent + norm_backward(back_two, second_normed, second_inv, gain_two)
    middle_feed = middle_grad.astype(jnp.bfloat16)
    grad_bias_out = jnp.sum(middle_grad, axis=0)
    attended_grad = jnp.einsum(
        "te,de->td", middle_feed, weight_out, preferred_element_type=jnp.float32
    ).astype(jnp.bfloat16)
    query_grads, key_ext, value_ext = attend_back(
        token_bounds, queries, keys, values, attended_list, attended_grad, lse
    )
    ext_grad = jnp.concatenate([key_ext, value_ext], axis=1)
    device_count = n_dp * n_shard
    forward = [(i, (i + 1) % device_count) for i in range(device_count)]
    backward = [((i + 1) % device_count, i) for i in range(device_count)]
    from_after = lax.ppermute(ext_grad[:RIM], ("dp", "shard"), backward)
    from_before = lax.ppermute(
        lax.dynamic_slice_in_dim(ext_grad, RIM + live_count, RIM, 0), ("dp", "shard"), forward
    )
    spot = lax.axis_index(("dp", "shard"))
    from_before = jnp.where((spot > 0), from_before, 0.0)
    from_after = jnp.where((spot < device_count - 1), from_after, 0.0)
    own_grad = jnp.where(is_live[:, None], ext_grad[RIM : RIM + BLOCK], 0.0)
    own_grad = own_grad.at[:RIM].add(from_before)
    own_grad = jnp.pad(own_grad, ((16, 0), (0, 0)))
    at = live_count + 16 - RIM
    tail_now = lax.dynamic_slice_in_dim(own_grad, at, RIM, 0)
    own_grad = lax.dynamic_update_slice_in_dim(own_grad, tail_now + from_after, at, 0)[16:]
    grad_bias_q = jnp.sum(query_grads, axis=0)
    grad_bias_v = jnp.sum(own_grad[:, D:], axis=0)
    joined = jnp.concatenate([query_grads, own_grad], axis=1).astype(jnp.bfloat16)
    back_one = jnp.einsum("te,de->td", joined, weight_qkv, preferred_element_type=jnp.float32)
    grad_gain_one = jnp.sum(back_one * first_normed, axis=0)
    grad_shift_one = jnp.sum(back_one, axis=0)
    stream_grad = middle_grad + norm_backward(back_one, first_normed, first_inv, gain_one)
    input_grad = jnp.where(is_live[:, None], stream_grad, 0.0)
    vector_grad = jnp.stack(
        [
            grad_gain_one,
            grad_shift_one,
            grad_bias_q,
            grad_bias_v,
            grad_bias_out,
            grad_gain_two,
            grad_shift_two,
            grad_bias_back,
        ]
    )
    vector_lines = jnp.concatenate([vector_grad.reshape(-1), grad_bias_in]).reshape(-1, LANES)
    flat_grads = weight_grads(
        n_dp,
        n_shard,
        first_feed,
        joined,
        attended_list,
        middle_feed,
        second_feed,
        slope_feed,
        activated,
        tangent_b,
        vector_lines,
    )
    reduced = reduce_grads(n_dp, n_shard, flat_grads).reshape(-1)
    piece_len = own_len // n_dp
    grad_shard = reduced[:own_len].astype(jnp.float32)
    grad_piece = lax.dynamic_slice_in_dim(
        grad_shard, lax.axis_index("dp") * piece_len, piece_len, 0
    )
    matrices = 4 * D * D + 2 * D * FF
    global_ids = lax.axis_index("shard") * own_len + jnp.arange(own_len, dtype=jnp.int32)
    decays = (global_ids < matrices).astype(jnp.float32)
    new_first = beta_one * first_moment + (1.0 - beta_one) * grad_shard
    new_second = beta_two * second_moment + (1.0 - beta_two) * grad_shard * grad_shard
    first_hat = new_first / (1.0 - beta_one**3)
    second_hat = new_second / (1.0 - beta_two**3)
    new_params = params - learn_rate * (
        first_hat / (jnp.sqrt(second_hat) + adam_eps) + decay_rate * decays * params
    )
    param_grad = grad_piece.reshape(1, 1, piece_len)
    return (activations, input_grad, param_grad, new_params, new_first, new_second)


def solution(mesh):
    in_specs = (
        P(("dp", "shard"), None),
        P(("dp", "shard"), None),
        P(("dp", "shard"), None),
        P("shard"),
        P("shard"),
        P("shard"),
    )
    out_specs = (
        P(("dp", "shard"), None),
        P(("dp", "shard"), None),
        P("shard", "dp", None),
        P("shard"),
        P("shard"),
        P("shard"),
    )
    return jax.shard_map(shards, mesh=mesh, in_specs=in_specs, out_specs=out_specs, check_vma=False)
```

```python
import functools

import jax
import jax.numpy as jnp
from jax import lax
from jax.experimental import pallas as pl
from jax.experimental.pallas import tpu as pltpu
from jax.sharding import PartitionSpec as P

D = 768
HEADS = 12
HD = 64
FF = 3072
IMG = 197
BLOCK = 512


ln_eps = 1e-06
masked = -1e30
beta_one = 0.9
beta_two = 0.999
learn_rate = 0.02
decay_rate = 0.05
adam_eps = 1e-08
sqrt_half = 0.7071067811865476
inv_root_two_pi = 0.3989422804014327


MESH = pl.DeviceIdType.MESH
LANES = 128
MARGIN = 64


def geometry(n_dp, n_shard):
    total = 4 * D * D + 2 * D * FF + 8 * D + FF
    shard_lines = total // n_shard // LANES
    piece = -(-(-(-shard_lines // n_dp)) // 64) * 64
    return shard_lines, piece, piece * n_dp


def bit_list(n_dp):
    count = n_dp.bit_length() - 1
    return count, [list(range(1, count)), list(range(count - 1, 0, -1))]


def bits_of(index, count):
    return [lax.rem(lax.div(index, 1 << b), 2) for b in range(count)]


def flipped(index, bits, which):
    return index + sum((1 << b) * (1 - 2 * bits[b]) for b in which)


def greet(n_dp, n_shard, place, level, bits, extra=()):
    barrier = pltpu.get_barrier_semaphore()
    peers = [(place, lax.rem(level + j, n_shard)) for j in range(1, n_shard)]
    peers += [(flipped(place, bits, [b]), level) for b in range(len(bits))]
    peers += list(extra)
    for peer in peers:
        pl.semaphore_signal(barrier, inc=1, device_id=peer, device_id_type=MESH)
    pl.semaphore_wait(barrier, len(peers))


def subsets(order):
    found = [[]]
    for b in order:
        found = found + [kept + [b] for kept in found]
    return found


def ring(n_dp, n_shard, place, level):
    spot = place * n_shard + level
    size = n_dp * n_shard
    sides = [lax.rem(spot + size - 1, size), lax.rem(spot + 1, size)]
    return [(lax.div(side, n_shard), lax.rem(side, n_shard)) for side in sides]


def gather_kernel(
    n_dp, n_shard, half, own, head, tail, out, before, after, z_send, z_recv, d_send, d_recv, r_send, r_recv
):
    place = lax.axis_index("dp")
    level = lax.axis_index("shard")
    count, orders = bit_list(n_dp)
    bits = bits_of(place, count)
    previous, following = ring(n_dp, n_shard, place, level)
    greet(n_dp, n_shard, place, level, bits, (previous, following))
    started = []

    def push(src, dst, send, recv, target):
        copy = pltpu.make_async_remote_copy(
            src_ref=src,
            dst_ref=dst,
            send_sem=send,
            recv_sem=recv,
            device_id=target,
            device_id_type=MESH,
        )
        copy.start()
        started.append(copy)

    push(head, after, r_send.at[0], r_recv.at[0], previous)
    push(tail, before, r_send.at[1], r_recv.at[1], following)
    for side in range(2):
        for j in range(1, n_shard):
            push(
                own.at[place, side],
                out.at[level, place, side],
                z_send.at[j - 1, side],
                z_recv.at[j - 1, side],
                (place, lax.rem(level + j, n_shard)),
            )
    chunks = [(j, side) for j in range(1, n_shard) for side in range(2)]

    def advance(chunk, stage):
        j, side = chunks[chunk]
        source = lax.rem(level - j + n_shard, n_shard)
        order = orders[side] + [0]

        def arrived(piece, sem):
            pltpu.make_async_remote_copy(
                src_ref=own.at[place, side],
                dst_ref=out.at[source, piece, side],
                send_sem=z_send.at[0, 0],
                recv_sem=sem,
                device_id=(place, level),
                device_id_type=MESH,
            ).wait_recv()

        if stage == 0:
            arrived(place, z_recv.at[j - 1, side])
        else:
            partner = flipped(place, bits, [order[stage - 1]])
            for slot, which in enumerate(subsets(order[: stage - 1])):
                arrived(
                    flipped(place, bits, which + [order[stage - 1]]),
                    d_recv.at[chunk, (1 << (stage - 1)) - 1 + slot],
                )
        if stage < count:
            partner = flipped(place, bits, [order[stage]])
            for slot, which in enumerate(subsets(order[:stage])):
                piece = flipped(place, bits, which)
                index = (1 << stage) - 1 + slot
                push(
                    out.at[source, piece, side],
                    out.at[source, piece, side],
                    d_send.at[chunk, index],
                    d_recv.at[chunk, index],
                    (partner, level),
                )

    for tick in range(len(chunks) + count):
        for stage in range(count + 1):
            chunk = tick - stage
            if 0 <= chunk < len(chunks):
                advance(chunk, stage)
    started[0].wait_recv()
    started[1].wait_recv()
    for copy in started:
        copy.wait_send()


def gather_weights(n_dp, n_shard, own, head, tail):
    shard_lines, piece, padded = geometry(n_dp, n_shard)
    half = piece // 2
    chunks = 2 * (n_shard - 1)
    space = pl.BlockSpec(memory_space=pltpu.HBM)
    return pl.pallas_call(
        functools.partial(gather_kernel, n_dp, n_shard, half),
        out_shape=[
            jax.ShapeDtypeStruct((n_shard, n_dp, 2, half, LANES), jnp.bfloat16),
            jax.ShapeDtypeStruct((RIM, D), jnp.bfloat16),
            jax.ShapeDtypeStruct((RIM, D), jnp.bfloat16),
        ],
        in_specs=[space] * 3,
        out_specs=[space] * 3,
        scratch_shapes=[
            pltpu.SemaphoreType.DMA((n_shard - 1, 2)),
            pltpu.SemaphoreType.DMA((n_shard - 1, 2)),
            pltpu.SemaphoreType.DMA((chunks, n_dp - 1)),
            pltpu.SemaphoreType.DMA((chunks, n_dp - 1)),
            pltpu.SemaphoreType.DMA((2,)),
            pltpu.SemaphoreType.DMA((2,)),
        ],
        compiler_params=pltpu.CompilerParams(collective_id=1, has_side_effects=True),
        name="gather_weights",
    )(own, head, tail)


def weight_plan(n_shard, shard_lines):
    sizes = [(D, 3 * D), (D, D), (D, FF), (FF, D)]
    plan = [[] for _ in range(n_shard)]
    cursor = 0
    for which, (rows, columns) in enumerate(sizes):
        width = columns // LANES
        first = 0
        for s in range(n_shard):
            stop = (s + 1) * shard_lines
            last = min(rows, max(first, (stop - cursor) // width))
            last = last if last == rows else last // 128 * 128
            if last > first:
                plan[s].append((which, first, last, width, cursor + first * width - s * shard_lines))
                first = last
        cursor += rows * width
    return plan, cursor


def layout_kernel(n_shard, shard_lines, padded, own, got, wqkv, wout, win, wback, vec, raw, wide, sem):
    level = lax.axis_index("shard")
    plan, tail = weight_plan(n_shard, shard_lines)
    targets = [wqkv, wout, win, wback]

    def load(s, slot):
        @pl.when(level == s)
        def _():
            pltpu.make_async_copy(own, raw.at[slot], sem.at[slot]).start()

        @pl.when(level != s)
        def _():
            pltpu.make_async_copy(got.at[s], raw.at[slot], sem.at[slot]).start()

    load(0, 0)
    for s in range(n_shard):
        slot = s % 2
        pltpu.make_async_copy(own, raw.at[slot], sem.at[slot]).wait()
        if s + 1 < n_shard:
            load(s + 1, 1 - slot)
        if s:
            wide[0:MARGIN, :] = wide[shard_lines : shard_lines + MARGIN, :]

        def spread(i, carry):
            at = pl.multiple_of(i * 128, 128)
            wide[pl.ds(MARGIN + at, 128), :] = raw[slot, pl.ds(at, 128), :].astype(jnp.float32)
            return carry

        lax.fori_loop(0, padded // 128, spread, 0)
        for which, first, last, width, offset in plan[s]:
            target = targets[which]

            def rows(i, carry):
                at = pl.multiple_of(first + i * 16, 16)
                line = MARGIN + offset + i * (16 * width)
                for c in range(width):
                    target[pl.ds(at, 16), c * LANES : (c + 1) * LANES] = wide[
                        pl.ds(line + c, 16, stride=width), :
                    ].astype(jnp.bfloat16)
                return carry

            lax.fori_loop(0, (last - first) // 16, rows, 0)
    start = MARGIN + tail - (n_shard - 1) * shard_lines
    vec[...] = wide[start : start + vec.shape[0], :]


def lay_out_weights(n_dp, n_shard, own, got):
    shard_lines, piece, padded = geometry(n_dp, n_shard)
    count = (8 * D + FF) // LANES
    shapes = [(D, 3 * D), (D, D), (D, FF), (FF, D)]
    return pl.pallas_call(
        functools.partial(layout_kernel, n_shard, shard_lines, padded),
        out_shape=[jax.ShapeDtypeStruct(shape, jnp.bfloat16) for shape in shapes]
        + [jax.ShapeDtypeStruct((count, LANES), jnp.float32)],
        in_specs=[pl.BlockSpec(memory_space=pltpu.HBM)] * 2,
        out_specs=[pl.BlockSpec(memory_space=pltpu.VMEM)] * 5,
        scratch_shapes=[
            pltpu.VMEM((2, padded, LANES), jnp.bfloat16),
            pltpu.VMEM((MARGIN + padded, LANES), jnp.float32),
            pltpu.SemaphoreType.DMA((2,)),
        ],
        compiler_params=pltpu.CompilerParams(vmem_limit_bytes=60 << 20),
        name="lay_out_weights",
    )(own.reshape(padded, LANES), got.reshape(n_shard, padded, LANES))


RIM = 208
EXT = 1024
QB = 128
WIN = 640


def window_bias(start, block):
    inv = 1.0 / IMG
    rows = lax.broadcasted_iota(jnp.int32, (QB, 1), 0) + (start + block * QB)
    cols = lax.broadcasted_iota(jnp.int32, (1, WIN), 1) + (start - RIM + block * QB)
    row_image = jnp.floor((rows.astype(jnp.float32) + 0.5) * inv)
    col_image = jnp.floor((cols.astype(jnp.float32) + 0.5) * inv)
    return jnp.where(row_image == col_image, 0.0, masked)


def stacked(rows):
    lane = lax.broadcasted_iota(jnp.int32, (QB, LANES), 1)
    zero = jnp.zeros_like(rows)
    return jnp.concatenate([jnp.where(lane < HD, rows, zero), jnp.where(lane < HD, zero, rows)], axis=0)


def unstacked(rows):
    lane = lax.broadcasted_iota(jnp.int32, (QB, LANES), 1)
    return jnp.where(lane < HD, rows[:QB], rows[QB:])


def attend_kernel(bounds, rows, weight, vectors, feed, queries, keys, values, attended, lse, wide_feed, bias):
    start = bounds[0, 0]
    gain, shift = vectors[0:1, :], vectors[1:2, :]

    def norm(i, carry):
        at = pl.multiple_of(i * 64, 64)
        x = rows[pl.ds(at, 64), :].astype(jnp.float32)
        centred = x - jnp.mean(x, axis=-1, keepdims=True)
        inverse = lax.rsqrt(jnp.mean(centred * centred, axis=-1, keepdims=True) + ln_eps)
        wide_feed[pl.ds(at, 64), :] = (centred * inverse * gain + shift).astype(jnp.bfloat16)
        return carry

    lax.fori_loop(0, EXT // 64, norm, 0)
    feed[...] = wide_feed[RIM : RIM + BLOCK, :]

    def project(i, carry):
        at = pl.multiple_of(i * 256, 256)
        block = wide_feed[pl.ds(at, 256), :]
        keys[pl.ds(at, 256), :] = jnp.dot(
            block, weight[:, D : 2 * D], preferred_element_type=jnp.float32
        ).astype(jnp.bfloat16)
        values[pl.ds(at, 256), :] = (
            jnp.dot(block, weight[:, 2 * D :], preferred_element_type=jnp.float32) + vectors[3:4, :]
        ).astype(jnp.bfloat16)
        return carry

    lax.fori_loop(0, EXT // 256, project, 0)

    def ask(i, carry):
        at = pl.multiple_of(i * 256, 256)
        queries[pl.ds(at, 256), :] = (
            (jnp.dot(feed[pl.ds(at, 256), :], weight[:, :D], preferred_element_type=jnp.float32) + vectors[2:3, :])
            * 0.125
        ).astype(jnp.bfloat16)
        return carry

    lax.fori_loop(0, BLOCK // 256, ask, 0)
    for block in range(BLOCK // QB):
        bias[block] = window_bias(start, block)

    def attend(i, carry):
        block = lax.rem(i, BLOCK // QB)
        pair = lax.div(i, BLOCK // QB)
        at = pl.multiple_of(block * QB, QB)
        lanes = pl.ds(pl.multiple_of(pair * LANES, LANES), LANES)
        scores = lax.dot_general(
            stacked(queries[pl.ds(at, QB), lanes]),
            keys[pl.ds(at, WIN), lanes],
            (((1,), (1,)), ((), ())),
            preferred_element_type=jnp.float32,
        )
        cover = bias[block]
        scores = scores + jnp.concatenate([cover, cover], axis=0)
        top = jnp.max(scores, axis=-1, keepdims=True)
        raised = jnp.exp(scores - top)
        total = jnp.sum(raised, axis=-1, keepdims=True)
        probs = (raised * (1.0 / total)).astype(jnp.bfloat16)
        out = jnp.dot(probs, values[pl.ds(at, WIN), lanes], preferred_element_type=jnp.float32)
        attended[pl.ds(at, QB), lanes] = unstacked(out).astype(jnp.bfloat16)
        lse[pair, block] = jnp.broadcast_to(top + jnp.log(total), (2 * QB, LANES))
        return carry

    lax.fori_loop(0, HEADS // 2 * (BLOCK // QB), attend, 0)


def attend(bounds, rows, weight, vectors):
    half = jnp.bfloat16
    return pl.pallas_call(
        attend_kernel,
        out_shape=[
            jax.ShapeDtypeStruct((BLOCK, D), half),
            jax.ShapeDtypeStruct((BLOCK, D), half),
            jax.ShapeDtypeStruct((EXT, D), half),
            jax.ShapeDtypeStruct((EXT, D), half),
            jax.ShapeDtypeStruct((BLOCK, D), half),
            jax.ShapeDtypeStruct((HEADS // 2, BLOCK // QB, 2 * QB, LANES), jnp.float32),
        ],
        in_specs=[pl.BlockSpec(memory_space=pltpu.SMEM)] + [pl.BlockSpec(memory_space=pltpu.VMEM)] * 3,
        out_specs=[pl.BlockSpec(memory_space=pltpu.VMEM)] * 6,
        scratch_shapes=[
            pltpu.VMEM((EXT, D), half),
            pltpu.VMEM((BLOCK // QB, QB, WIN), jnp.float32),
        ],
        compiler_params=pltpu.CompilerParams(vmem_limit_bytes=60 << 20),
        name="attend",
    )(bounds, rows, weight, vectors)


def wide_plan(n_shard, shard_lines):
    sizes = [(D, 3 * D), (D, D), (D, FF), (FF, D)]
    plan = [[] for _ in range(n_shard)]
    cursor = 0
    for which, (rows, columns) in enumerate(sizes):
        width = columns // LANES
        for s in range(n_shard):
            begin, stop = s * shard_lines, (s + 1) * shard_lines
            first = max(0, (begin - cursor) // width)
            last = min(rows, -(-(stop - cursor) // width))
            if last > first:
                plan[s].append((which, first // 128 * 128, last, width, cursor - begin))
        cursor += rows * width
    return plan, cursor - (n_shard - 1) * shard_lines


def fill_lines(wide, left, right, first, last, width, offset):
    def product(row, group):
        return lax.dot_general(
            left[:, pl.ds(row, 128)],
            right[:, group * 768 : (group + 1) * 768],
            (((0,), (0,)), ((), ())),
            preferred_element_type=jnp.float32,
        )

    def store(row, count):
        line = MARGIN + offset + row * width
        for group in range(width // 6):
            tile = product(row, group)
            for c in range(6):
                wide[pl.ds(line + group * 6 + c, count, stride=width), :] = tile[
                    :count, c * LANES : (c + 1) * LANES
                ]

    full = (last - first) // 128

    def block(i, carry):
        store(pl.multiple_of(first + i * 128, 128), 128)
        return carry

    if full:
        lax.fori_loop(0, full, block, 0)
    row = first + full * 128
    rest = -(-(last - row) // 8) * 8
    if rest:
        store(row, rest)


class Links:
    def __init__(self, n_dp, n_shard):
        self.n_dp, self.n_shard = n_dp, n_shard
        self.place = lax.axis_index("dp")
        self.level = lax.axis_index("shard")
        self.count, self.orders = bit_list(n_dp)
        self.bits = bits_of(self.place, self.count)
        self.sent = []

    def push(self, src, dst, send, recv, target):
        pltpu.make_async_remote_copy(
            src_ref=src,
            dst_ref=dst,
            send_sem=send,
            recv_sem=recv,
            device_id=target,
            device_id_type=MESH,
        ).start()

    def note(self, refs, when=None):
        self.sent.append((refs, when))

    def landed(self, buffer, sem):
        pltpu.make_async_remote_copy(
            src_ref=buffer,
            dst_ref=buffer,
            send_sem=sem,
            recv_sem=sem,
            device_id=self.over(0),
            device_id_type=MESH,
        ).wait_recv()

    def over(self, bit):
        return (flipped(self.place, self.bits, [bit]), self.level)

    def drain(self):
        for refs, when in self.sent:

            def wait(refs=refs):
                src, send = refs()
                pltpu.make_async_remote_copy(
                    src_ref=src,
                    dst_ref=src,
                    send_sem=send,
                    recv_sem=send,
                    device_id=self.over(0),
                    device_id_type=MESH,
                ).wait_send()

            if when is None:
                wait()
            else:
                pl.when(when)(wait)


class PlaneSum:
    def __init__(self, links, wide, part, bufs):
        self.links, self.wide, self.part = links, wide, part
        self.core_got, self.core_send, self.core_recv, self.send_bufs, self.got_bufs, self.bit_send, self.bit_recv = bufs
        self.lines = self.core_got.shape[-2]
        self.pairs = links.n_dp // 2

    def rows(self, piece, quarter):
        return pl.ds(pl.multiple_of(MARGIN + (piece * 4 + quarter) * self.lines, 8), self.lines)

    def begin(self):
        links = self.links
        core = links.bits[0]
        for quarter in range(4):
            for m in range(self.pairs):
                src = self.wide.at[self.rows(2 * m + 1 - core, quarter)]
                send = self.core_send.at[self.part, quarter, m]
                links.push(
                    src,
                    self.core_got.at[self.part, quarter, m],
                    send,
                    self.core_recv.at[self.part, quarter, m],
                    links.over(0),
                )
                links.note(
                    lambda quarter=quarter, m=m: (
                        self.core_got.at[self.part, quarter, m],
                        self.core_send.at[self.part, quarter, m],
                    )
                )

    def members(self, order, stage, flip):
        bits = self.links.bits
        base = sum((bits[b] if b != flip else 1 - bits[b]) * (1 << (b - 1)) for b in order[:stage])
        return [base + sum(1 << (b - 1) for b in which) for which in subsets(order[stage:])]

    def merge(self, piece, quarter, other, into):
        step = 112
        start = MARGIN + (piece * 4 + quarter) * self.lines

        def body(i, carry):
            at = pl.multiple_of(i * step, 16)
            rows = pl.ds(pl.multiple_of(start + at, 8), step)
            total = self.wide[rows, :] + other[pl.ds(at, step), :].astype(jnp.float32)
            if into is None:
                self.wide[rows, :] = total
            else:
                into[pl.ds(at, step), :] = total.astype(into.dtype)
            return carry

        lax.fori_loop(0, self.lines // step, body, 0)

    def advance(self, quarter, stage, result=None):
        links, part = self.links, self.part
        core = links.bits[0]
        order = links.orders[quarter % 2]

        def incoming(slot, m):
            if stage == 0:
                return self.core_got.at[part, quarter, m], self.core_recv.at[part, quarter, m]
            return (
                self.got_bufs[stage - 1].at[part, quarter, slot],
                self.bit_recv.at[stage - 1, part, quarter, slot],
            )

        if stage == links.count - 1:
            (m,) = self.members(order, stage, None)
            buffer, sem = incoming(0, m)
            links.landed(buffer, sem)
            self.merge(2 * m + core, quarter, buffer, result)
            return
        flip = order[stage]
        mine = links.bits[flip]
        for flipping in (True, False):
            bit = 1 - mine if flipping else mine
            for e, m in enumerate(self.members(order, stage + 1, flip if flipping else None)):
                buffer, sem = incoming(2 * e + bit, m)
                links.landed(buffer, sem)
                if flipping:
                    out = self.send_bufs[stage].at[part, quarter, e]
                    self.merge(2 * m + core, quarter, buffer, out)
                    send = self.bit_send.at[stage, part, quarter, e]
                    links.push(
                        out,
                        self.got_bufs[stage].at[part, quarter, e],
                        send,
                        self.bit_recv.at[stage, part, quarter, e],
                        links.over(flip),
                    )
                    links.note(
                        lambda stage=stage, e=e: (
                            self.send_bufs[stage].at[part, quarter, e],
                            self.bit_send.at[stage, part, quarter, e],
                        )
                    )
                else:
                    self.merge(2 * m + core, quarter, buffer, None)


def plane_scratch(n_dp, lines, parts):
    count = n_dp.bit_length() - 1
    pairs = n_dp // 2
    half = jnp.bfloat16
    stages = [pltpu.VMEM((parts, 4, pairs >> t, lines, LANES), half) for t in range(1, count)]
    return (
        [
            pltpu.VMEM((parts, 4, pairs, lines, LANES), jnp.float32),
            pltpu.SemaphoreType.DMA((parts, 4, pairs)),
            pltpu.SemaphoreType.DMA((parts, 4, pairs)),
        ]
        + stages
        + stages
        + [
            pltpu.SemaphoreType.DMA((count - 1, parts, 4, pairs // 2)),
            pltpu.SemaphoreType.DMA((count - 1, parts, 4, pairs // 2)),
        ]
    )


def plane_bufs(n_dp, scratch):
    count = n_dp.bit_length() - 1
    k = count - 1
    used = 3 + 2 * k + 2
    core_got, core_send, core_recv = scratch[:3]
    bufs = (core_got, core_send, core_recv, scratch[3 : 3 + k], scratch[3 + k : 3 + 2 * k], *scratch[3 + 2 * k : used])
    return bufs, scratch[used:]


def back_kernel(n_dp, n_shard, lines, *refs):
    (bounds, feed_two, slope, activated, tangent, *attention) = refs[:11]
    joined, sums, plane = refs[11:14]
    bufs, rest = plane_bufs(n_dp, refs[14:])
    (wide_a, wide_b, queries, keys, values, attended, grads, lse, key_grad, value_grad, bias) = rest[:11]
    (out_rim, got_rim, padded_rim, load_sem, rim_send, rim_recv, plane_sem) = rest[11:]
    total_lines = (4 * D * D + 2 * D * FF + 8 * D + FF) // n_shard // LANES
    links = Links(n_dp, n_shard)
    place, level = links.place, links.level
    previous, following = ring(n_dp, n_shard, place, level)
    targets = [queries, keys, values, attended, grads, lse]
    loads = [
        pltpu.make_async_copy(src, dst, load_sem.at[i]) for i, (src, dst) in enumerate(zip(attention, targets))
    ]
    for load in loads:
        load.start()
    greet(n_dp, n_shard, place, level, links.bits, (previous, following))
    plan, tail = wide_plan(n_shard, total_lines)
    lefts = [None, None, feed_two, activated]
    rights = [None, None, slope, tangent]
    early = [PlaneSum(links, wide_a, 0, bufs), PlaneSum(links, wide_b, 1, bufs)]

    def fill(wide, entry):
        which, first, last, width, offset = entry
        fill_lines(wide, lefts[which], rights[which], first, last, width, offset)

    for entry in plan[n_shard - 1]:
        fill(wide_a, entry)
    early[0].begin()
    second = plan[n_shard - 2]
    fill(wide_b, second[0])
    for quarter in range(4):
        early[0].advance(quarter, 0)
    for entry in second[1:]:
        fill(wide_b, entry)
    early[1].begin()
    for load in loads:
        load.wait()
    start = bounds[0, 0]
    live = bounds[0, 1] - bounds[0, 0]
    blocks = BLOCK // QB
    for block in range(blocks):
        bias[block] = window_bias(start, block)
    key_grad[...] = jnp.zeros_like(key_grad)
    value_grad[...] = jnp.zeros_like(value_grad)
    sums[...] = jnp.zeros_like(sums)
    last_stage = links.count - 1
    chain = []
    for part in range(2):
        for quarter in range(4):
            for stage in range(1 if part == 0 else 0, last_stage):
                chain.append((4 + 9 * part + 2.5 * quarter + (stage - 1) * 8 + (3 if part else 0), part, quarter, stage))
    ticks = {}
    for when, part, quarter, stage in sorted(chain):
        ticks.setdefault(min(int(when), 23), []).append((part, quarter, stage))

    def send_rim(pair):
        for kind, source in enumerate((key_grad, value_grad)):
            base = pair * EXT
            out_rim[0, pair, kind] = source[pl.ds(pl.multiple_of(base, EXT), RIM), :].astype(jnp.bfloat16)
            out_rim[1, pair, kind] = source[pl.ds(base + RIM + live, RIM), :].astype(jnp.bfloat16)
        for side, target in enumerate((previous, following)):
            links.push(
                out_rim.at[side, pair], got_rim.at[side, pair], rim_send.at[side, pair], rim_recv.at[side, pair], target
            )

    def body(i, carry):
        block = lax.rem(i, blocks)
        pair = lax.div(i, blocks)
        at = pl.multiple_of(block * QB, QB)
        lanes = pl.ds(pl.multiple_of(pair * LANES, LANES), LANES)
        asked = stacked(queries[pl.ds(at, QB), lanes])
        given = stacked(grads[pl.ds(at, QB), lanes])
        near = pl.ds(pl.multiple_of(pair * EXT + at, QB), WIN)
        near_keys = keys[pl.ds(at, WIN), lanes]
        near_values = values[pl.ds(at, WIN), lanes]
        scores = lax.dot_general(
            asked, near_keys, (((1,), (1,)), ((), ())), preferred_element_type=jnp.float32
        )
        cover = bias[block]
        height = lse[pair, block]
        probs = jnp.exp(
            scores + jnp.concatenate([cover, cover], axis=0) - jnp.concatenate([height] * (WIN // LANES), axis=1)
        )
        prob_grad = lax.dot_general(
            given, near_values, (((1,), (1,)), ((), ())), preferred_element_type=jnp.float32
        )
        both = given.astype(jnp.float32) * jnp.concatenate([attended[pl.ds(at, QB), lanes]] * 2, axis=0).astype(
            jnp.float32
        )
        centre = jnp.sum(both, axis=-1, keepdims=True)
        score_grad = (probs * (prob_grad - centre)).astype(jnp.bfloat16)
        query_grad = unstacked(jnp.dot(score_grad, near_keys, preferred_element_type=jnp.float32)) * 0.125
        joined[pl.ds(at, QB), lanes] = query_grad.astype(jnp.bfloat16)
        sums[0:1, lanes] += jnp.sum(query_grad, axis=0, keepdims=True)
        key_grad[near, :] += lax.dot_general(
            score_grad, asked, (((0,), (0,)), ((), ())), preferred_element_type=jnp.float32
        )
        value_grad[near, :] += lax.dot_general(
            probs.astype(jnp.bfloat16), given, (((0,), (0,)), ((), ())), preferred_element_type=jnp.float32
        )

        @pl.when(block == blocks - 1)
        def _():
            send_rim(pair)

        for key, work in ticks.items():

            @pl.when(i == key)
            def _(work=work):
                for part, quarter, stage in work:
                    early[part].advance(quarter, stage)

        return carry

    lax.fori_loop(0, HEADS // 2 * blocks, body, 0)
    for side in range(2):
        for pair in range(HEADS // 2):
            links.note(lambda side=side, pair=pair: (out_rim.at[side, pair], rim_send.at[side, pair]))
    spot = place * n_shard + level
    padded_rim[...] = jnp.zeros_like(padded_rim)
    chunk = 64

    def settle(pair, carry):
        links.landed(got_rim.at[0, pair], rim_recv.at[0, pair])
        links.landed(got_rim.at[1, pair], rim_recv.at[1, pair])
        at_pair = pl.multiple_of(pair * LANES, LANES)
        base = pair * EXT
        for kind, source in enumerate((key_grad, value_grad)):
            after = got_rim[0, pair, kind].astype(jnp.float32)
            padded_rim[BLOCK : BLOCK + RIM, :] = jnp.where(spot < n_dp * n_shard - 1, after, 0.0)

            def rows(r, inner):
                at = pl.multiple_of(r * chunk, chunk)
                slot = lax.broadcasted_iota(jnp.int32, (chunk, 1), 0) + at
                own = source[pl.ds(pl.multiple_of(base + RIM + at, 16), chunk), :]
                own = jnp.where(slot < live, own, 0.0)
                own = own + padded_rim[pl.ds(BLOCK + RIM - live + at, chunk), :]
                source[pl.ds(pl.multiple_of(base + RIM + at, 16), chunk), :] = own
                return inner

            lax.fori_loop(0, BLOCK // chunk, rows, 0)
            before = got_rim[1, pair, kind].astype(jnp.float32)
            head = source[pl.ds(pl.multiple_of(base + RIM, 16), RIM), :] + jnp.where(spot > 0, before, 0.0)
            source[pl.ds(pl.multiple_of(base + RIM, 16), RIM), :] = head
            own = source[pl.ds(pl.multiple_of(base + RIM, 16), BLOCK), :]
            joined[:, pl.ds(pl.multiple_of((1 + kind) * D + at_pair, LANES), LANES)] = own.astype(jnp.bfloat16)
            if kind:
                sums[1:2, pl.ds(at_pair, LANES)] = jnp.sum(own, axis=0, keepdims=True)
        return carry

    lax.fori_loop(0, HEADS // 2, settle, 0)
    for part in range(2):
        for quarter in range(4):
            early[part].advance(quarter, last_stage)
            piece = links.place
            pltpu.make_async_copy(
                early[part].wide.at[early[part].rows(piece, quarter)],
                plane.at[1 - part, quarter],
                plane_sem.at[part, quarter],
            ).start()
    for part in range(2):
        for quarter in range(4):
            pltpu.make_async_copy(
                early[part].wide.at[early[part].rows(links.place, quarter)],
                plane.at[1 - part, quarter],
                plane_sem.at[part, quarter],
            ).wait()
    links.drain()


def back_attention(n_dp, n_shard, bounds, feed_two, slope, activated, tangent, *attention):
    shard_lines, piece, padded = geometry(n_dp, n_shard)
    lines = piece // 4
    half = jnp.bfloat16
    vmem = pl.BlockSpec(memory_space=pltpu.VMEM)
    hbm = pl.BlockSpec(memory_space=pltpu.HBM)
    pairs = HEADS // 2
    wide = pltpu.VMEM((MARGIN + padded + 128, LANES), jnp.float32)
    return pl.pallas_call(
        functools.partial(back_kernel, n_dp, n_shard, lines),
        out_shape=[
            jax.ShapeDtypeStruct((BLOCK, 3 * D), half),
            jax.ShapeDtypeStruct((8, D), jnp.float32),
            jax.ShapeDtypeStruct((2, 4, lines, LANES), jnp.float32),
        ],
        in_specs=[pl.BlockSpec(memory_space=pltpu.SMEM)] + [vmem] * 4 + [hbm] * 6,
        out_specs=[vmem, vmem, hbm],
        scratch_shapes=plane_scratch(n_dp, lines, 2)
        + [wide, wide]
        + [pltpu.VMEM(a.shape, a.dtype) for a in attention]
        + [
            pltpu.VMEM((pairs * EXT, LANES), jnp.float32),
            pltpu.VMEM((pairs * EXT, LANES), jnp.float32),
            pltpu.VMEM((BLOCK // QB, QB, WIN), jnp.float32),
            pltpu.VMEM((2, pairs, 2, RIM, LANES), half),
            pltpu.VMEM((2, pairs, 2, RIM, LANES), half),
            pltpu.VMEM((2 * BLOCK + RIM + 64, LANES), jnp.float32),
            pltpu.SemaphoreType.DMA((6,)),
            pltpu.SemaphoreType.DMA((2, pairs)),
            pltpu.SemaphoreType.DMA((2, pairs)),
            pltpu.SemaphoreType.DMA((2, 4)),
        ],
        compiler_params=pltpu.CompilerParams(
            collective_id=2, has_side_effects=True, vmem_limit_bytes=63 << 20
        ),
        name="back_attention",
    )(bounds, feed_two, slope, activated, tangent, *attention)


def finish_kernel(n_dp, n_shard, lines, *refs):
    (joined, feed_one, attended, middle, feed_two, slope, early_plane, vec) = refs[:8]
    out, vec_out = refs[8:10]
    bufs, rest = plane_bufs(n_dp, refs[10:])
    wide_a, wide_b, plane, z_out, z_got, final, vec_got, vec_work = rest[:8]
    plane_sem, z_send, z_recv, g_send, g_recv, keep_sem, v_send, v_recv = rest[8:]
    total_lines = (4 * D * D + 2 * D * FF + 8 * D + FF) // n_shard // LANES
    links = Links(n_dp, n_shard)
    place, level, count = links.place, links.level, links.count
    step = 112
    plane_load = pltpu.make_async_copy(
        early_plane, plane.at[pl.ds(n_shard - 2, 2)], plane_sem.at[0]
    )
    plane_load.start()
    greet(n_dp, n_shard, place, level, links.bits)
    plan, tail = wide_plan(n_shard, total_lines)
    lefts = [feed_one, attended, feed_two, None]
    rights = [joined, middle, slope, None]
    late = [PlaneSum(links, wide_b, 0, bufs), PlaneSum(links, wide_a, 1, bufs)]

    def fill(wide, entry):
        which, first, last, width, offset = entry
        fill_lines(wide, lefts[which], rights[which], first, last, width, offset)

    def gathered(parts):
        def body(i, carry):
            at = pl.multiple_of(i * step, 16)
            total = parts[0][pl.ds(at, step), :].astype(jnp.float32)
            for other in parts[1:-1]:
                total = total + other[pl.ds(at, step), :].astype(jnp.float32)
            parts[-1][pl.ds(at, step), :] = total.astype(jnp.bfloat16)
            return carry

        lax.fori_loop(0, lines // step, body, 0)

    def chain(s, quarter, k):
        for below in (True, False):
            actor = k if below else n_shard - 1 - k
            if (actor >= s) if below else (actor <= s):
                continue
            side = 0 if below else 1

            @pl.when(level == actor)
            def _(side=side, below=below):
                parts = [plane.at[s, quarter]]
                if k:
                    links.landed(z_got.at[s, quarter, side], z_recv.at[s, quarter, side])
                    parts.append(z_got.at[s, quarter, side])
                gathered(parts + [z_out.at[s, quarter]])
                links.push(
                    z_out.at[s, quarter],
                    z_got.at[s, quarter, side],
                    z_send.at[s, quarter],
                    z_recv.at[s, quarter, side],
                    (place, level + (1 if below else -1)),
                )

        if k == max(s, n_shard - 1 - s):

            @pl.when(level == s)
            def _():
                parts = [plane.at[s, quarter]]
                for side, there in ((0, s > 0), (1, s < n_shard - 1)):
                    if there:
                        links.landed(z_got.at[s, quarter, side], z_recv.at[s, quarter, side])
                        parts.append(z_got.at[s, quarter, side])
                gathered(parts + [final.at[quarter]])

    for s in range(n_shard):
        for quarter in range(4):
            links.note(lambda s=s, quarter=quarter: (z_out.at[s, quarter], z_send.at[s, quarter]), level != s)

    def spread(quarter, stage):
        order = links.orders[quarter % 2] + [0]
        if stage == 0:
            pltpu.make_async_copy(final.at[quarter], out.at[place, quarter], keep_sem.at[quarter]).start()
        else:
            for slot, which in enumerate(subsets(order[: stage - 1])):
                piece = flipped(place, links.bits, which + [order[stage - 1]])
                links.landed(out.at[piece, quarter], g_recv.at[quarter, (1 << (stage - 1)) - 1 + slot])
        if stage < count:
            for slot, which in enumerate(subsets(order[:stage])):
                piece = flipped(place, links.bits, which)
                index = (1 << stage) - 1 + slot
                src = final.at[quarter] if not which else out.at[piece, quarter]
                links.push(
                    src, out.at[piece, quarter], g_send.at[quarter, index], g_recv.at[quarter, index], links.over(order[stage])
                )
                links.note(lambda index=index: (final.at[quarter], g_send.at[quarter, index]))

    def share(stage):
        if stage == 0:
            vec_work[0] = vec[...]
        elif stage <= count:
            links.landed(vec_got.at[stage - 1], v_recv.at[stage - 1])
            vec_work[stage] = vec_work[stage - 1] + vec_got[stage - 1]
        if stage < count:
            links.push(vec_work.at[stage], vec_got.at[stage], v_send.at[stage], v_recv.at[stage], links.over(stage))
            links.note(lambda: (vec_work.at[stage], v_send.at[stage]))
        elif stage == count:
            for j in range(1, n_shard):
                links.push(
                    vec_work.at[count],
                    vec_got.at[count + j - 1],
                    v_send.at[count + j - 1],
                    v_recv.at[count + j - 1],
                    (place, lax.rem(level + j, n_shard)),
                )
                links.note(lambda j=j: (vec_work.at[count], v_send.at[count + j - 1]))
        else:
            total = vec_work[count]
            for j in range(1, n_shard):
                links.landed(vec_got.at[count + j - 1], v_recv.at[count + j - 1])
                total = total + vec_got[count + j - 1]
            vec_out[...] = total

    last_stage = count - 1
    work = []
    for quarter in range(4):
        for k in range(n_shard):
            work.append((2.5 * quarter + 6 * k, "z", n_shard - 1, quarter, k))
            work.append((10 + 2.5 * quarter + 6 * k, "z", n_shard - 2, quarter, k))
            work.append((26.5 + 2.5 * quarter + 4 * k, "z", 1, quarter, k))
            work.append((39.5 + 2.5 * quarter + 4 * k, "z", 0, quarter, k))
        for stage in range(count):
            work.append((12 + 2.5 * quarter + 7 * stage, "p", 0, quarter, stage))
            work.append((21 + 2.5 * quarter + 9 * stage, "p", 1, quarter, stage))
        for stage in range(count + 1):
            work.append((52 + 2.5 * quarter + 4 * stage, "g", 0, quarter, stage))
    for stage in range(count + 2):
        work.append((3 + 5 * stage, "v", 0, 0, stage))
    work.sort()

    def run_until(limit):
        while work and work[0][0] < limit:
            when, kind, a, quarter, stage = work.pop(0)
            if kind == "z":
                chain(a, quarter, stage)
            elif kind == "p":
                late[a].advance(quarter, stage, plane.at[1 - a, quarter] if stage == last_stage else None)
            elif kind == "g":
                spread(quarter, stage)
            else:
                share(stage)

    fill(wide_b, plan[1][0])
    plane_load.wait()
    run_until(4)
    for entry in plan[1][1:]:
        fill(wide_b, entry)
    late[0].begin()
    run_until(8)
    for entry in plan[0]:
        which, first, last, width, offset = entry
        middle_row = (first + last) // 256 * 128
        if which == 0 and middle_row > first:
            fill(wide_a, (which, first, middle_row, width, offset))
            run_until(13)
            fill(wide_a, (which, middle_row, last, width, offset))
        else:
            fill(wide_a, entry)
    late[1].begin()
    run_until(1 << 30)
    for quarter in range(4):
        pltpu.make_async_copy(final.at[quarter], out.at[place, quarter], keep_sem.at[quarter]).wait()
    links.drain()


def finish_grads(n_dp, n_shard, *operands):
    shard_lines, piece, padded = geometry(n_dp, n_shard)
    lines = piece // 4
    count = n_dp.bit_length() - 1
    half = jnp.bfloat16
    vmem = pl.BlockSpec(memory_space=pltpu.VMEM)
    hbm = pl.BlockSpec(memory_space=pltpu.HBM)
    wide = pltpu.VMEM((MARGIN + padded + 128, LANES), jnp.float32)
    vec = operands[-1].shape
    return pl.pallas_call(
        functools.partial(finish_kernel, n_dp, n_shard, lines),
        out_shape=[
            jax.ShapeDtypeStruct((n_dp, 4, lines, LANES), half),
            jax.ShapeDtypeStruct(vec, jnp.float32),
        ],
        in_specs=[vmem] * 6 + [hbm, vmem],
        out_specs=[hbm, vmem],
        scratch_shapes=plane_scratch(n_dp, lines, 2)
        + [
            wide,
            wide,
            pltpu.VMEM((n_shard, 4, lines, LANES), jnp.float32),
            pltpu.VMEM((n_shard, 4, lines, LANES), half),
            pltpu.VMEM((n_shard, 4, 2, lines, LANES), half),
            pltpu.VMEM((4, lines, LANES), half),
            pltpu.VMEM((count + n_shard - 1, *vec), jnp.float32),
            pltpu.VMEM((count + 1, *vec), jnp.float32),
            pltpu.SemaphoreType.DMA((1,)),
            pltpu.SemaphoreType.DMA((n_shard, 4)),
            pltpu.SemaphoreType.DMA((n_shard, 4, 2)),
            pltpu.SemaphoreType.DMA((4, n_dp - 1)),
            pltpu.SemaphoreType.DMA((4, n_dp - 1)),
            pltpu.SemaphoreType.DMA((4,)),
            pltpu.SemaphoreType.DMA((count + n_shard - 1,)),
            pltpu.SemaphoreType.DMA((count + n_shard - 1,)),
        ],
        compiler_params=pltpu.CompilerParams(
            collective_id=3, has_side_effects=True, vmem_limit_bytes=63 << 20
        ),
        name="finish_grads",
    )(*operands)


def gelu_value(preact):
    return 0.5 * preact * (1.0 + lax.erf(preact * sqrt_half))


def gelu_slope(preact):
    return (
        0.5 * (1.0 + lax.erf(preact * sqrt_half))
        + preact * jnp.exp(-0.5 * preact * preact) * inv_root_two_pi
    )


def norm_stats(values):
    centred = values - jnp.mean(values, axis=-1, keepdims=True)
    inverse = lax.rsqrt(jnp.mean(centred * centred, axis=-1, keepdims=True) + ln_eps)
    return centred * inverse, inverse


def norm_forward(values, gain_vec, shift_vec):
    centre = jnp.mean(values, axis=-1, keepdims=True)
    centred = values - centre
    spread = jnp.mean(centred * centred, axis=-1, keepdims=True)
    inverse = lax.rsqrt(spread + ln_eps)
    normed = centred * inverse
    return (normed * gain_vec + shift_vec, normed, inverse)


def norm_backward(upstream, normed, inverse, gain_vec):
    scaled = upstream * gain_vec
    first_mean = jnp.mean(scaled, axis=-1, keepdims=True)
    second = jnp.mean(scaled * normed, axis=-1, keepdims=True)
    return inverse * (scaled - first_mean - normed * second)


def shards(block_input, cotangent, token_bounds, params, first_moment, second_moment):
    rows_here = block_input.shape[0]
    own_len = params.shape[0]
    n_dp, n_shard = lax.axis_size("dp"), lax.axis_size("shard")
    shard_lines, piece, padded = geometry(n_dp, n_shard)
    own_weights = jnp.pad(params.astype(jnp.bfloat16), (0, padded * LANES - own_len)).reshape(
        n_dp, 2, piece // 2, LANES
    )
    live_count = token_bounds[0, 1] - token_bounds[0, 0]
    tail_rows = lax.dynamic_slice_in_dim(jnp.pad(block_input, ((16, 0), (0, 0))), live_count + (16 - RIM), RIM, 0)
    gathered, before, after = gather_weights(n_dp, n_shard, own_weights, block_input[:RIM], tail_rows)
    weight_qkv, weight_out, weight_in, weight_back, lines = lay_out_weights(
        n_dp, n_shard, own_weights, gathered
    )
    vector_f = lines[: 8 * D // LANES].reshape(8, D)
    bias_in = lines[8 * D // LANES :].reshape(FF)
    gain_one, shift_one, bias_q, bias_v = (vector_f[0], vector_f[1], vector_f[2], vector_f[3])
    bias_out, gain_two, shift_two, bias_back = (vector_f[4], vector_f[5], vector_f[6], vector_f[7])
    slot_ids = jnp.arange(rows_here, dtype=jnp.int32)
    is_live = slot_ids < live_count
    stream = block_input.astype(jnp.float32)
    first_normed, first_inv = norm_stats(stream)
    wide_rows = jnp.concatenate(
        [before, block_input, jnp.zeros((EXT - RIM - BLOCK, D), jnp.bfloat16)], axis=0
    )
    wide_rows = lax.dynamic_update_slice_in_dim(wide_rows, after, RIM + live_count, 0)
    first_feed, queries, keys, values, attended_list, lse = attend(
        token_bounds, wide_rows, weight_qkv, vector_f
    )
    middle = (
        stream + jnp.dot(attended_list, weight_out, preferred_element_type=jnp.float32) + bias_out
    )
    second_out, second_normed, second_inv = norm_forward(middle, gain_two, shift_two)
    second_feed = second_out.astype(jnp.bfloat16)
    preact = jnp.dot(second_feed, weight_in, preferred_element_type=jnp.float32) + bias_in
    activated = gelu_value(preact).astype(jnp.bfloat16)
    result = (
        middle + jnp.dot(activated, weight_back, preferred_element_type=jnp.float32) + bias_back
    )
    activations = jnp.where(is_live[:, None], result, 0.0)
    tangent_b = jnp.where(is_live[:, None], cotangent, jnp.zeros_like(cotangent))
    tangent = tangent_b.astype(jnp.float32)
    grad_bias_back = jnp.sum(tangent, axis=0)
    slope_in = jnp.einsum(
        "td,fd->tf", tangent_b, weight_back, preferred_element_type=jnp.float32
    ) * gelu_slope(preact)
    grad_bias_in = jnp.sum(slope_in, axis=0)
    slope_feed = slope_in.astype(jnp.bfloat16)
    back_two = jnp.einsum("tf,df->td", slope_feed, weight_in, preferred_element_type=jnp.float32)
    grad_gain_two = jnp.sum(back_two * second_normed, axis=0)
    grad_shift_two = jnp.sum(back_two, axis=0)
    middle_grad = tangent + norm_backward(back_two, second_normed, second_inv, gain_two)
    middle_feed = middle_grad.astype(jnp.bfloat16)
    grad_bias_out = jnp.sum(middle_grad, axis=0)
    attended_grad = jnp.einsum(
        "te,de->td", middle_feed, weight_out, preferred_element_type=jnp.float32
    ).astype(jnp.bfloat16)
    joined, sums, plane = back_attention(
        n_dp,
        n_shard,
        token_bounds,
        second_feed,
        slope_feed,
        activated,
        tangent_b,
        queries,
        keys,
        values,
        attended_list,
        attended_grad,
        lse,
    )
    grad_bias_q, grad_bias_v = sums[0], sums[1]
    back_one = jnp.einsum("te,de->td", joined, weight_qkv, preferred_element_type=jnp.float32)
    grad_gain_one = jnp.sum(back_one * first_normed, axis=0)
    grad_shift_one = jnp.sum(back_one, axis=0)
    stream_grad = middle_grad + norm_backward(back_one, first_normed, first_inv, gain_one)
    input_grad = jnp.where(is_live[:, None], stream_grad, 0.0)
    vector_grad = jnp.stack(
        [
            grad_gain_one,
            grad_shift_one,
            grad_bias_q,
            grad_bias_v,
            grad_bias_out,
            grad_gain_two,
            grad_shift_two,
            grad_bias_back,
        ]
    )
    vector_lines = jnp.concatenate([vector_grad.reshape(-1), grad_bias_in]).reshape(-1, LANES)
    reduced, vector_sum = finish_grads(
        n_dp,
        n_shard,
        joined,
        first_feed,
        attended_list,
        middle_feed,
        second_feed,
        slope_feed,
        plane,
        vector_lines,
    )
    reduced = reduced.reshape(-1)
    piece_len = own_len // n_dp
    grad_shard = reduced[:own_len].astype(jnp.float32)
    vector_len = 8 * D + FF
    with_vectors = jnp.concatenate([grad_shard[: own_len - vector_len], vector_sum.reshape(-1)])
    grad_shard = jnp.where(lax.axis_index("shard") == n_shard - 1, with_vectors, grad_shard)
    grad_piece = lax.dynamic_slice_in_dim(
        grad_shard, lax.axis_index("dp") * piece_len, piece_len, 0
    )
    matrices = 4 * D * D + 2 * D * FF
    global_ids = lax.axis_index("shard") * own_len + jnp.arange(own_len, dtype=jnp.int32)
    decays = (global_ids < matrices).astype(jnp.float32)
    new_first = beta_one * first_moment + (1.0 - beta_one) * grad_shard
    new_second = beta_two * second_moment + (1.0 - beta_two) * grad_shard * grad_shard
    first_hat = new_first / (1.0 - beta_one**3)
    second_hat = new_second / (1.0 - beta_two**3)
    new_params = params - learn_rate * (
        first_hat / (jnp.sqrt(second_hat) + adam_eps) + decay_rate * decays * params
    )
    param_grad = grad_piece.reshape(1, 1, piece_len)
    return (activations, input_grad, param_grad, new_params, new_first, new_second)


def solution(mesh):
    in_specs = (
        P(("dp", "shard"), None),
        P(("dp", "shard"), None),
        P(("dp", "shard"), None),
        P("shard"),
        P("shard"),
        P("shard"),
    )
    out_specs = (
        P(("dp", "shard"), None),
        P(("dp", "shard"), None),
        P("shard", "dp", None),
        P("shard"),
        P("shard"),
        P("shard"),
    )
    return jax.shard_map(shards, mesh=mesh, in_specs=in_specs, out_specs=out_specs, check_vma=False)
```
